128 devices in a mesh: grp: 2 (over core), dom: 64 (over x, z, y).
Axes of the slice: x: 4, y: 4, z: 4, core: 2. Of those that a mesh axis runs over, the one named last changes fastest.
Arguments:
- flow_temp: float32 [128, 2048, 256], P(None, ('grp', 'dom')), may hold values from -6 to 6
- velocity: bfloat16 [3, 128, 2048, 256], P(None, None, ('grp', 'dom')), may hold values from -2.5 to 2.5
- heat_release: bfloat16 [128, 2048, 256], P(None, ('grp', 'dom')), may hold values from 0.049804688 to 2
- solid_temp: float32 [32, 2048, 256], P(None, ('grp', 'dom')), may hold values from -6 to 6
- conductivity: float32 [32, 2048, 256], P(None, ('grp', 'dom')), may hold values from 0.5 to 2
- interp_table: float32 [16, 16, 1024], replicated, may hold values from -0.375 to 0.375
- flow_patch: int32 [524288], P(('grp', 'dom')), may hold values from 0 to 255
- solid_device: int32 [524288, 1], P(('grp', 'dom')), may hold values from 0 to 127; in each aligned block of 4096 rows (0 to 4095, 4096 to 8191, ...) at most 64 rows name the same one
- solid_patch: int32 [524288], P(('grp', 'dom')), may hold values from 0 to 255
- block_index: int32 [524288], P(('grp', 'dom')), may hold values from 0 to 1023
Outputs:
- flow_out: float32 [128, 2048, 256], P(None, ('grp', 'dom'))
- solid_out: float32 [32, 2048, 256], P(None, ('grp', 'dom'))
The draws below stay inside these ranges and needn't reach their ends.
Inputs may be any that keep to these rules, and one draw needn't show every extreme that they name: `solid_device`: within the 4096 rows of one device no liner device is named more than 64 times, and some liner device is named exactly 64 times.
All inputs are finite; a program needn't handle non-finite values.
Results may differ from the reference program's by a relative error of at most 0.00115.
Values may be sent and summed in bfloat16 or wider, within the bound.
A program may use at most 128 MiB of HBM per device.

```python
import math
import jax
import jax.numpy as jnp
import numpy as np
from jax import lax

NY = 256
NZF = 128
NZS = 32
SUBCYCLES = 4
NB = 1024
PF = 256
OV_DEV = 4096
CAP = 64
NXF = 2048
PATCHES = 32768
CORRELATIONS = 524288
N_GRP = 2
N_DOM = 64
DEVICES = 128


def place_ends(array, stream_key, low, largest):
    dims = array.shape
    place = [jax.random.randint(jax.random.fold_in(stream_key, axis), (), 0, dims[axis]) for axis in range(len(dims))]
    array = array.at[tuple(place)].set(low)
    longest = dims.index(max(dims))
    place[longest] = (place[longest] + 1) % dims[longest]
    return array.at[tuple(place)].set(largest)


def shard_levels(rng, dims, cuts, smallest, top_value):
    factor_of = 1.0
    for position, blocks in cuts:
        draws = jax.random.uniform(jax.random.fold_in(jax.random.fold_in(rng, 6), position), (blocks,), jnp.float32, smallest / len(cuts), top_value / len(cuts))
        factor_of = factor_of * jnp.repeat(jnp.exp(draws), dims[position] // blocks).reshape((-1,) + (1,) * (len(dims) - 1 - position))
    return factor_of


def deal_out(own_key, own, number, rows, amount, top, reach, lean):
    ranking = jax.random.permutation(own_key, amount)
    heavy_load, ordinary = load_shares(amount, rows * top, reach, lean, True), load_shares(amount, rows * top, reach, lean, False)
    places = jnp.arange(amount)

    def named(lengths, rotation):
        used = int((lengths > 0).sum())
        fixed = max(1, used // 4)
        passed = fixed + (places - fixed + rotation * (used - fixed)) % max(1, amount - fixed)
        return jnp.zeros((amount,), jnp.int32).at[ranking[jnp.where(places < fixed, places, passed)]].set(jnp.asarray(lengths, jnp.int32))

    lengths = jnp.where(number % 4 == 0, named(heavy_load, number // 4), named(ordinary, number - number // 4 - 1))
    mixed = jax.random.permutation(jax.random.fold_in(own, 3), amount)
    giver, sink = mixed[0:amount // 2 * 2:2], mixed[1:amount // 2 * 2:2]
    slack = jnp.minimum(lengths[giver] - 1, reach - lengths[sink]) // 2
    slack = jnp.where((giver == ranking[0]) | (sink == ranking[0]) | (lengths[sink] == 0), 0, jnp.maximum(slack, 0))
    passed = jax.random.randint(jax.random.fold_in(own, 4), (amount // 2,), 0, 1 << 20) % (slack + 1)
    lengths = lengths.at[giver].add(-passed).at[sink].add(passed)
    members = jnp.searchsorted(jnp.cumsum(lengths), jnp.arange(rows * top), side="right").astype(jnp.int32)
    table = members.reshape(top, rows).T
    table = table[jax.random.permutation(jax.random.fold_in(own, 1), rows)]
    rotation = jax.random.randint(jax.random.fold_in(own, 2), (rows, 1), 0, top)
    return jnp.take_along_axis(table, (jnp.arange(top)[None, :] + rotation) % top, axis=1)


def load_shares(amount, total, limit, lean, full):
    portions = [(1 << 20) // math.isqrt(rank ** lean) + 1 for rank in range(1, amount + 1)]
    largest = limit if full else min(limit, max(-(-total // amount), total * portions[0] // sum(portions)))
    least = 1 if total - largest >= amount - 1 else 0
    holding, surplus = [largest] + [least] * (amount - 1), total - largest - least * (amount - 1)
    while surplus > 0:
        free = [i for i in range(1, amount) if holding[i] < largest] or [i for i in range(1, amount) if holding[i] < limit]
        whole, budget = sum([portions[i] for i in free]), surplus
        for i in free:
            more = min(limit - holding[i], max(1, budget * portions[i] // whole), surplus)
            holding[i] = holding[i] + more
            surplus = surplus - more
    return np.array(holding)


def noise(rng, shape, deviation, limit, cuts=(), kind=jnp.bfloat16):
    result = jax.random.normal(rng, shape, jnp.float32) * deviation
    if len(cuts) > 0:
        result = shard_levels(rng, shape, cuts, -0.22, 0.18) * result
    return jnp.clip(result, min=-limit, max=limit).astype(kind)


def setup_inputs(seed: int = 0) -> dict:
    key_of = jax.random.split(jax.random.key(seed), 11)
    flow_temp = noise(key_of[0], (NZF, NXF, NY), 1.0, 6.0, ((1, 128),), jnp.float32)
    velocity = noise(key_of[1], (3, NZF, NXF, NY), 0.7, 2.5, ((2, 128),))
    heat_release = jnp.clip(jnp.exp(math.log(2.0) - 3.6927934 * jax.random.uniform(key_of[2], (NZF, NXF, NY), jnp.float32) ** shard_levels(key_of[2], (NZF, NXF, NY), ((1, 128),), -0.2, 0.2)), 0.049804688, 2.0).astype(jnp.bfloat16)
    solid_temp = noise(key_of[3], (NZS, NXF, NY), 1.0, 6.0, ((1, 128),), jnp.float32)
    conductivity = jnp.clip(jnp.exp(math.log(2.0) - 1.3862944 * jax.random.uniform(key_of[4], (NZS, NXF, NY), jnp.float32) ** shard_levels(key_of[4], (NZS, NXF, NY), ((1, 128),), -0.2, 0.2)), 0.5, 2.0)
    interp_table = noise(key_of[5], (16, 16, NB), 256 ** -0.5, 0.375, (), jnp.float32)
    flow_patch = place_ends(jax.random.randint(key_of[6], (CORRELATIONS,), 0, PF), jax.random.fold_in(key_of[6], 1), 0, PF - 1).astype(jnp.int32)
    solid_device_keys = jax.random.split(jax.random.fold_in(key_of[7], 1), CORRELATIONS // OV_DEV)
    solid_device_turns = jax.random.permutation(jax.random.fold_in(key_of[7], 3), CORRELATIONS // OV_DEV)
    solid_device = jax.vmap(lambda own, number: deal_out(jax.random.fold_in(key_of[7], 2), own, number, OV_DEV, DEVICES, 1, CAP, 2))(solid_device_keys, solid_device_turns).reshape((CORRELATIONS, 1))
    solid_patch = place_ends(jax.random.randint(key_of[8], (CORRELATIONS,), 0, PF), jax.random.fold_in(key_of[8], 1), 0, PF - 1).astype(jnp.int32)
    block_index = place_ends(jax.random.randint(key_of[9], (CORRELATIONS,), 0, NB), jax.random.fold_in(key_of[9], 1), 0, NB - 1).astype(jnp.int32)
    return {"flow_temp": flow_temp, "velocity": velocity, "heat_release": heat_release, "solid_temp": solid_temp, "conductivity": conductivity, "interp_table": interp_table, "flow_patch": flow_patch, "solid_device": solid_device, "solid_patch": solid_patch, "block_index": block_index}


DIFFUSION = 0.8
TIMESTEP = 0.12
FILM_COEFF = 1.0
CONDUCT_RATE = 0.08
FLUX_GAIN = 0.25
slab_depth = 8


def to_patches(face_values):
    rows_x, cols_y = face_values.shape
    return face_values.reshape(rows_x, cols_y // 16, 16).transpose(2, 0, 1).reshape(16, rows_x * (cols_y // 16))


def from_patches(patches, rows_x):
    per_row = patches.shape[1] // rows_x
    return patches.reshape(16, rows_x, per_row).transpose(1, 2, 0).reshape(rows_x, per_row * 16)


def upwind(component, centre, lower_side, upper_side):
    return jnp.maximum(component, 0.0) * (centre - lower_side) + jnp.minimum(component, 0.0) * (upper_side - centre)


def tendency(centre, zbelow, zabove, xbelow, xabove, velocity, source):
    ybelow = jnp.roll(centre, 1, axis=2)
    yabove = jnp.roll(centre, -1, axis=2)
    advect = upwind(velocity[0], centre, zbelow, zabove) + upwind(velocity[1], centre, xbelow, xabove)
    advect = advect + upwind(velocity[2], centre, ybelow, yabove)
    spread = zbelow + zabove + xbelow + xabove + ybelow + yabove - 6.0 * centre
    return source - advect + DIFFUSION * spread


def flow_tendency(current, wall_face, velocity, heat_release):
    padded = jnp.concatenate([jnp.zeros_like(current[:1]), current, wall_face[None]], 0)

    def compute_slab(offset):
        slab_rows = lax.dynamic_slice_in_dim(padded, offset, slab_depth + 2, 0)
        centre = slab_rows[1:-1]
        speeds = lax.dynamic_slice_in_dim(velocity, offset, slab_depth, 1).astype(jnp.float32)
        source = lax.dynamic_slice_in_dim(heat_release, offset, slab_depth, 0).astype(jnp.float32)
        return tendency(centre, slab_rows[:-2], slab_rows[2:], jnp.roll(centre, 1, axis=1), jnp.roll(centre, -1, axis=1), speeds, source)

    offsets = jnp.arange(NZF // slab_depth, dtype=jnp.int32) * slab_depth
    return lax.map(compute_slab, offsets).reshape(current.shape)


def solid_update(current, xbelow, xabove, conduct, flux_face):
    zbelow = jnp.concatenate([current[:1], current[:-1]], 0)
    zabove = jnp.concatenate([current[1:], jnp.zeros_like(current[:1])], 0)
    ybelow = jnp.roll(current, 1, axis=2)
    yabove = jnp.roll(current, -1, axis=2)
    spread = zbelow + zabove + xbelow + xabove + ybelow + yabove - 6.0 * current
    updated = current + CONDUCT_RATE * conduct * spread
    return updated + jnp.concatenate([(FLUX_GAIN * flux_face)[None], jnp.zeros_like(current[1:])], 0)


def reference(flow_temp, velocity, heat_release, solid_temp, conductivity, interp_table, flow_patch, solid_device, solid_patch, block_index):
    devices = N_GRP * N_DOM
    owners = jnp.arange(CORRELATIONS, dtype=jnp.int32) // OV_DEV
    flow_index = (owners * PF + flow_patch).astype(jnp.int32)
    solid_index = (solid_device[:, 0] * PF + solid_patch).astype(jnp.int32)
    solid_wall = to_patches(solid_temp[0])

    def forward_block(pieces):
        blocks, places = pieces
        weights = jnp.take(interp_table, blocks, axis=2)
        return jnp.sum(weights * jnp.take(solid_wall, places, axis=1)[None, :, :], axis=1)

    forward = lax.map(forward_block, (block_index.reshape(devices, OV_DEV), solid_index.reshape(devices, OV_DEV)))
    forward = jnp.transpose(forward, (1, 0, 2)).reshape(16, CORRELATIONS)
    wall_temp = jnp.zeros((16, PATCHES), jnp.float32).at[:, flow_index].add(forward)
    wall_face = from_patches(wall_temp, NXF)
    predictor = flow_temp + TIMESTEP * flow_tendency(flow_temp, wall_face, velocity, heat_release)
    flow_out = 0.5 * flow_temp + 0.5 * (predictor + TIMESTEP * flow_tendency(predictor, wall_face, velocity, heat_release))
    wall_flux = to_patches(FILM_COEFF * (flow_out[-1] - wall_face))

    def backward_block(pieces):
        blocks, places = pieces
        weights = jnp.take(interp_table, blocks, axis=2)
        return jnp.sum(weights * jnp.take(wall_flux, places, axis=1)[:, None, :], axis=0)

    backward = lax.map(backward_block, (block_index.reshape(devices, OV_DEV), flow_index.reshape(devices, OV_DEV)))
    backward = jnp.transpose(backward, (1, 0, 2)).reshape(16, CORRELATIONS)
    solid_flux = jnp.zeros((16, PATCHES), jnp.float32).at[:, solid_index].add(backward)
    flux_face = from_patches(solid_flux, NXF)
    current = solid_temp
    for substep in range(SUBCYCLES):
        current = solid_update(current, jnp.roll(current, 1, axis=1), jnp.roll(current, -1, axis=1), conductivity, flux_face)
    return flow_out, current
```

```python
import functools

import jax
import jax.numpy as jnp
from jax import lax
from jax.experimental import pallas as pl
from jax.experimental.pallas import tpu as pltpu
from jax.sharding import PartitionSpec as P

MESH = pl.DeviceIdType.MESH
F32, BF16, I32 = jnp.float32, jnp.bfloat16, jnp.int32

SUBCYCLES = 4
DIFFUSION = 0.8
TIMESTEP = 0.12
FILM_COEFF = 1.0
CONDUCT_RATE = 0.08
FLUX_GAIN = 0.25

DEV = 128
KT = 256
NK = 4096
TILES = NK // KT
NN = (((1,), (0,)), ((), ()))
NT = (((1,), (1,)), ((), ()))

VMEM = pl.BlockSpec(memory_space=pltpu.VMEM)


def dot(a, b, dims=NN):
    return lax.dot_general(a, b, dims, preferred_element_type=F32)


def onehot(row, rows, base=0):
    place = lax.broadcasted_iota(I32, (rows, row.shape[1]), 0) + base
    return jnp.where(place == row, 1.0, 0.0).astype(BF16)


def split(value):
    high = value.astype(BF16)
    return high, (value - high.astype(F32)).astype(BF16)


def params(**more):
    return pltpu.CompilerParams(vmem_limit_bytes=60 * 1024 * 1024, **more)


def prep_kernel(flow, solid, cond, sd_ref, sp_ref, fe, se, wall, rank, ids, carry, acc):
    wall[...] = solid[0].astype(BF16)

    @pl.loop(0, 8)
    def _(b):
        z0 = pl.multiple_of(b * 16, 16)
        block = flow[pl.ds(z0, 16)]
        fe[0, pl.ds(z0, 16), :] = block[:, 0, :].astype(BF16)
        fe[1, pl.ds(z0, 16), :] = block[:, 15, :].astype(BF16)

    low = jnp.concatenate([solid[:, 0:4, :], cond[:, 0:4, :]], axis=1)
    high = jnp.concatenate([solid[:, 12:16, :], cond[:, 12:16, :]], axis=1)
    se[0] = low.reshape(16, 16, 256).astype(BF16)
    se[1] = high.reshape(16, 16, 256).astype(BF16)

    before = lax.broadcasted_iota(I32, (KT, KT), 0) < lax.broadcasted_iota(I32, (KT, KT), 1)
    before = jnp.where(before, 1.0, 0.0).astype(BF16)
    every = jnp.ones((KT, KT), BF16)
    carry[...] = jnp.zeros_like(carry)
    acc[...] = jnp.zeros_like(acc)

    @pl.loop(0, TILES)
    def _(t):
        k = pl.ds(pl.multiple_of(t * KT, KT), KT)
        sd = sd_ref[:, k]
        mine = lax.broadcasted_iota(I32, (DEV, KT), 0) == sd
        one = jnp.where(mine, 1.0, 0.0).astype(BF16)
        ahead = dot(one, before) + carry[...]
        r = jnp.sum(jnp.where(mine, ahead, 0.0), axis=0, keepdims=True).astype(I32)
        carry[...] += dot(one, every)
        rank[:, k] = r
        tag = (sp_ref[:, k] + 1).astype(F32)
        place = lax.broadcasted_iota(I32, (64, KT), 0)
        m = jnp.where(place == sd % 64, tag, 0.0).astype(BF16)
        a = (sd // 64) * 128 + r
        slot = (onehot(a, 256).astype(F32) + onehot(a + 64, 256).astype(F32)).astype(BF16)
        acc[...] += dot(m, slot, NT)

    got = acc[...]
    ids[0:64] = got[:, 0:128].reshape(64, 1, 128)
    ids[64:128] = got[:, 128:256].reshape(64, 1, 128)


def prep(flow, solid, cond, sd, sp):
    return pl.pallas_call(
        prep_kernel,
        out_shape=(
            jax.ShapeDtypeStruct((2, 128, 256), BF16),
            jax.ShapeDtypeStruct((2, 16, 16, 256), BF16),
            jax.ShapeDtypeStruct((16, 256), BF16),
            jax.ShapeDtypeStruct((1, NK), I32),
            jax.ShapeDtypeStruct((DEV, 1, 128), F32),
        ),
        in_specs=[VMEM] * 5,
        out_specs=(VMEM,) * 5,
        scratch_shapes=[pltpu.VMEM((DEV, KT), F32), pltpu.VMEM((64, 256), F32)],
        compiler_params=params(),
        name="prep",
    )(flow, solid, cond, sd, sp)


def where_am_i():
    return lax.axis_index("grp") * 64 + lax.axis_index("dom")


def coords(device):
    return (device // 64, device % 64)


def greet_all(me):
    barrier = pltpu.get_barrier_semaphore()

    @pl.loop(1, DEV)
    def _(o):
        pl.semaphore_signal(barrier, inc=1, device_id=coords((me + o) % DEV), device_id_type=MESH)

    pl.semaphore_wait(barrier, DEV - 1)


def greet_pair(me):
    barrier = pltpu.get_barrier_semaphore()
    for o in (1, DEV - 1):
        pl.semaphore_signal(barrier, inc=1, device_id=coords((me + o) % DEV), device_id_type=MESH)
    pl.semaphore_wait(barrier, 2)


def remote(src, dst, send, recv, device):
    return pltpu.make_async_remote_copy(
        src_ref=src,
        dst_ref=dst,
        send_sem=send,
        recv_sem=recv,
        device_id=coords(device),
        device_id_type=MESH,
    )


def pair_copies(me, edges, halo, send, recv):
    up = remote(edges.at[1], halo.at[0], send.at[0], recv.at[0], (me + 1) % DEV)
    down = remote(edges.at[0], halo.at[1], send.at[1], recv.at[1], (me + DEV - 1) % DEV)
    return up, down


def bulk_wait(ref, sem):
    many = ref.at[pl.ds(0, DEV - 1)]
    pltpu.make_async_copy(many, many, sem).wait()


def first_kernel(wall, ids, fe, se, ag, idr, fh, sh, send, recv, psend, precv):
    me = where_am_i()
    greet_all(me)
    pairs = pair_copies(me, fe, fh, psend.at[0], precv.at[0]) + pair_copies(
        me, se, sh, psend.at[1], precv.at[1]
    )
    for copy in pairs:
        copy.start()

    @pl.loop(1, DEV)
    def _(o):
        to = (me + o) % DEV
        remote(wall, ag.at[me], send.at[0], recv.at[0], to).start()
        remote(ids.at[to], idr.at[me], send.at[1], recv.at[1], to).start()

    ag[me] = wall[...]
    idr[me] = ids[me]
    for copy in pairs:
        copy.wait()
    bulk_wait(ag, recv.at[0])
    bulk_wait(idr, recv.at[1])
    bulk_wait(ag, send.at[0])
    bulk_wait(idr, send.at[1])


def first_exchange(wall, ids, fe, se):
    return pl.pallas_call(
        first_kernel,
        out_shape=(
            jax.ShapeDtypeStruct((DEV, 16, 256), BF16),
            jax.ShapeDtypeStruct((DEV, 1, 128), F32),
            jax.ShapeDtypeStruct(fe.shape, BF16),
            jax.ShapeDtypeStruct(se.shape, BF16),
        ),
        in_specs=[VMEM] * 4,
        out_specs=(VMEM,) * 4,
        scratch_shapes=[
            pltpu.SemaphoreType.DMA((2,)),
            pltpu.SemaphoreType.DMA((2,)),
            pltpu.SemaphoreType.DMA((2, 2)),
            pltpu.SemaphoreType.DMA((2, 2)),
        ],
        compiler_params=params(collective_id=0, has_side_effects=True),
        name="first_exchange",
    )(wall, ids, fe, se)


def pair_kernel(edges, halo, send, recv):
    me = where_am_i()
    greet_pair(me)
    pairs = pair_copies(me, edges, halo, send, recv)
    for copy in pairs:
        copy.start()
    for copy in pairs:
        copy.wait()


def pair_exchange(edges, number):
    return pl.pallas_call(
        pair_kernel,
        out_shape=jax.ShapeDtypeStruct(edges.shape, edges.dtype),
        in_specs=[VMEM],
        out_specs=VMEM,
        scratch_shapes=[pltpu.SemaphoreType.DMA((2,)), pltpu.SemaphoreType.DMA((2,))],
        compiler_params=params(collective_id=number, has_side_effects=True),
        name=f"pair_exchange_{number}",
    )(edges)


def slots_kernel(z, zr, send, recv):
    me = where_am_i()
    greet_all(me)

    @pl.loop(1, DEV)
    def _(o):
        to = (me + o) % DEV
        remote(z.at[to], zr.at[me], send, recv, to).start()

    zr[me] = z[me]
    bulk_wait(zr, recv)
    bulk_wait(zr, send)


def slots_exchange(z):
    return pl.pallas_call(
        slots_kernel,
        out_shape=jax.ShapeDtypeStruct(z.shape, z.dtype),
        in_specs=[VMEM],
        out_specs=VMEM,
        scratch_shapes=[pltpu.SemaphoreType.DMA, pltpu.SemaphoreType.DMA],
        compiler_params=params(collective_id=3, has_side_effects=True),
        name="slots_exchange",
    )(z)


def forward_kernel(tab_ref, ag, b_ref, fp_ref, sd_ref, sp_ref, wk, face, tab, lhs, acc):
    tab[0], tab[1] = split(tab_ref[...])
    for h in range(8):
        block = ag[h * 16 : (h + 1) * 16].reshape(256, 256)
        lhs[h * 256 : (h + 1) * 256] = block.astype(F32).T.astype(BF16)
    acc[...] = jnp.zeros_like(acc)

    @pl.loop(0, TILES)
    def _(t):
        k = pl.ds(pl.multiple_of(t * KT, KT), KT)
        b, fp, sd, sp = b_ref[:, k], fp_ref[:, k], sd_ref[:, k], sp_ref[:, k]
        block = onehot(b, 1024)
        w = dot(tab[0], block) + dot(tab[1], block)
        wk[:, k] = w
        pick = onehot((sd % 16) * 16 + sp // 16, 256)
        key = (sd // 16) * 16 + sp % 16
        x = jnp.zeros((16, KT), F32)
        for h in range(8):
            r = dot(lhs[h * 256 : (h + 1) * 256], pick)
            for c in range(16):
                x = jnp.where(key == h * 16 + c, r[c * 16 : (c + 1) * 16], x)
        y = jnp.concatenate(
            [jnp.sum(w[i * 16 : (i + 1) * 16] * x, axis=0, keepdims=True) for i in range(16)], axis=0
        )
        col = fp % 16
        spread = jnp.concatenate([jnp.where(col == c, y, 0.0) for c in range(16)], axis=0)
        high, low = split(spread)
        row = onehot(fp // 16, 16)
        acc[...] += dot(high, row, NT) + dot(low, row, NT)

    face[...] = acc[...].T


def forward(tab, ag, b, fp, sd, sp):
    return pl.pallas_call(
        forward_kernel,
        out_shape=(
            jax.ShapeDtypeStruct((256, NK), F32),
            jax.ShapeDtypeStruct((16, 256), F32),
        ),
        in_specs=[VMEM] * 6,
        out_specs=(VMEM,) * 2,
        scratch_shapes=[
            pltpu.VMEM((2, 256, 1024), BF16),
            pltpu.VMEM((2048, 256), BF16),
            pltpu.VMEM((256, 16), F32),
        ],
        compiler_params=params(),
        name="forward",
    )(tab, ag, b, fp, sd, sp)


def backward_kernel(flux, wk, fp_ref, sd_ref, rank, z, acc):
    fhigh, flow = split(flux[...].T)
    acc[...] = jnp.zeros_like(acc)

    @pl.loop(0, TILES)
    def _(t):
        k = pl.ds(pl.multiple_of(t * KT, KT), KT)
        fp, sd, r = fp_ref[:, k], sd_ref[:, k], rank[:, k]
        row = onehot(fp // 16, 16)
        g = dot(fhigh, row) + dot(flow, row)
        col = fp % 16
        y = jnp.zeros((16, KT), F32)
        for c in range(16):
            y = jnp.where(col == c, g[c * 16 : (c + 1) * 16], y)
        value = jnp.zeros((16, KT), F32)
        for i in range(16):
            value = value + wk[i * 16 : (i + 1) * 16, k] * y[i : i + 1]
        e = sd % 64
        a = (sd // 64) * 128 + r
        for h in range(2):
            half = value[h * 8 : (h + 1) * 8]
            m = jnp.concatenate([jnp.where(e == q, half, 0.0) for q in range(64)], axis=0)
            high, low = split(m)
            slot = onehot(a + 64 * h, 256)
            acc[...] += dot(high, slot, NT) + dot(low, slot, NT)

    got = acc[...]
    z[0:64] = got[:, 0:128].reshape(64, 8, 128)
    z[64:128] = got[:, 128:256].reshape(64, 8, 128)


def backward(flux, wk, fp, sd, rank):
    return pl.pallas_call(
        backward_kernel,
        out_shape=jax.ShapeDtypeStruct((DEV, 8, 128), F32),
        in_specs=[VMEM] * 5,
        out_specs=VMEM,
        scratch_shapes=[pltpu.VMEM((512, 256), F32)],
        compiler_params=params(),
        name="backward",
    )(flux, wk, fp, sd, rank)


def gather_up_kernel(zr, idr, edges, face, acc):
    acc[...] = jnp.zeros_like(acc)
    half = lax.broadcasted_iota(I32, (1, 128), 1) // 64

    @pl.loop(0, DEV // 4)
    def _(t):
        spreads, rows = [], []
        for q in range(4):
            s = t * 4 + q
            tag = idr[s].astype(I32) - 1
            key = jnp.where(tag < 0, -1, (tag % 16) * 2 + half)
            value = zr[s]
            spreads.append(
                jnp.concatenate([jnp.where(key == v, value, 0.0) for v in range(32)], axis=0)
            )
            rows.append(onehot(tag // 16, 16))
        high, low = split(jnp.concatenate(spreads, axis=1))
        row = jnp.concatenate(rows, axis=1)
        acc[...] += dot(high, row, NT) + dot(low, row, NT)

    total = acc[...].T * FLUX_GAIN
    face[...] = total
    edges[0] = total[0:4]
    edges[1] = total[12:16]


def gather_up(zr, idr):
    return pl.pallas_call(
        gather_up_kernel,
        out_shape=(
            jax.ShapeDtypeStruct((2, 4, 256), F32),
            jax.ShapeDtypeStruct((16, 256), F32),
        ),
        in_specs=[VMEM] * 2,
        out_specs=(VMEM,) * 2,
        scratch_shapes=[pltpu.VMEM((256, 16), F32)],
        compiler_params=params(),
        name="gather_up",
    )(zr, idr)


ZB = 16


def layer_tendency(centre, zbelow, zabove, xlow, xhigh, cz, cx, cy, source):
    rows = lax.broadcasted_iota(I32, (16, 256), 0)
    xbelow = jnp.where(rows == 0, xlow, pltpu.roll(centre, 1, 0))
    xabove = jnp.where(rows == 15, xhigh, pltpu.roll(centre, 15, 0))
    ybelow = pltpu.roll(centre, 1, 1)
    yabove = pltpu.roll(centre, 255, 1)
    total = source
    for c, below, above in ((cz, zbelow, zabove), (cx, xbelow, xabove), (cy, ybelow, yabove)):
        weight = jnp.maximum(c, 0.0) + DIFFUSION
        total = total + (below - centre) * weight + (above - centre) * (weight - c)
    return total


def predictor_kernel(flow, halo, wall, vel, heat, out, edge):
    b = pl.program_id(0)
    z0 = pl.multiple_of(b * ZB, ZB)
    xlow = halo[0, pl.ds(z0, ZB), :].astype(F32)
    xhigh = halo[1, pl.ds(z0, ZB), :].astype(F32)
    first, last = [], []
    for q in range(ZB):
        z = z0 + q
        centre = flow[z]
        zbelow = flow[z - 1] if q else jnp.where(b == 0, 0.0, flow[jnp.maximum(z - 1, 0)])
        if q < ZB - 1:
            zabove = flow[z + 1]
        else:
            zabove = jnp.where(b == 128 // ZB - 1, wall[...], flow[jnp.minimum(z + 1, 127)])
        slope = layer_tendency(
            centre,
            zbelow,
            zabove,
            xlow[q : q + 1],
            xhigh[q : q + 1],
            vel[0, q].astype(F32),
            vel[1, q].astype(F32),
            vel[2, q].astype(F32),
            heat[q].astype(F32),
        )
        value = centre + TIMESTEP * slope
        out[q] = value
        first.append(value[0:1])
        last.append(value[15:16])
    edge[0] = jnp.concatenate(first, axis=0).astype(BF16)
    edge[1] = jnp.concatenate(last, axis=0).astype(BF16)


def whole(*shape):
    return pl.BlockSpec(shape, lambda b: (0,) * len(shape))


def predictor(flow, halo, wall, vel, heat):
    return pl.pallas_call(
        predictor_kernel,
        grid=(128 // ZB,),
        out_shape=(
            jax.ShapeDtypeStruct((128, 16, 256), F32),
            jax.ShapeDtypeStruct((2, 128, 256), BF16),
        ),
        in_specs=[
            whole(128, 16, 256),
            whole(2, 128, 256),
            whole(16, 256),
            pl.BlockSpec((3, ZB, 16, 256), lambda b: (0, b, 0, 0)),
            pl.BlockSpec((ZB, 16, 256), lambda b: (b, 0, 0)),
        ],
        out_specs=(
            pl.BlockSpec((ZB, 16, 256), lambda b: (b, 0, 0)),
            pl.BlockSpec((2, ZB, 256), lambda b: (0, b, 0)),
        ),
        compiler_params=params(),
        name="predictor",
    )(flow, halo, wall, vel, heat)


def corrector_kernel(pred, halo, wall, vel, heat, flow, out, flux):
    b = pl.program_id(0)
    z0 = pl.multiple_of(b * ZB, ZB)
    xlow = halo[0, pl.ds(z0, ZB), :].astype(F32)
    xhigh = halo[1, pl.ds(z0, ZB), :].astype(F32)
    for q in range(ZB):
        z = z0 + q
        centre = pred[z]
        zbelow = pred[z - 1] if q else jnp.where(b == 0, 0.0, pred[jnp.maximum(z - 1, 0)])
        if q < ZB - 1:
            zabove = pred[z + 1]
        else:
            zabove = jnp.where(b == 128 // ZB - 1, wall[...], pred[jnp.minimum(z + 1, 127)])
        slope = layer_tendency(
            centre,
            zbelow,
            zabove,
            xlow[q : q + 1],
            xhigh[q : q + 1],
            vel[0, q].astype(F32),
            vel[1, q].astype(F32),
            vel[2, q].astype(F32),
            heat[q].astype(F32),
        )
        out[q] = 0.5 * flow[q] + 0.5 * (centre + TIMESTEP * slope)

    @pl.when(b == 128 // ZB - 1)
    def _():
        flux[...] = FILM_COEFF * (out[ZB - 1] - wall[...])


def corrector(pred, halo, wall, vel, heat, flow):
    return pl.pallas_call(
        corrector_kernel,
        grid=(128 // ZB,),
        out_shape=(
            jax.ShapeDtypeStruct((128, 16, 256), F32),
            jax.ShapeDtypeStruct((16, 256), F32),
        ),
        in_specs=[
            whole(128, 16, 256),
            whole(2, 128, 256),
            whole(16, 256),
            pl.BlockSpec((3, ZB, 16, 256), lambda b: (0, b, 0, 0)),
            pl.BlockSpec((ZB, 16, 256), lambda b: (b, 0, 0)),
            pl.BlockSpec((ZB, 16, 256), lambda b: (b, 0, 0)),
        ],
        out_specs=(
            pl.BlockSpec((ZB, 16, 256), lambda b: (b, 0, 0)),
            whole(16, 256),
        ),
        compiler_params=params(),
        name="corrector",
    )(pred, halo, wall, vel, heat, flow)


def solid_kernel(solid, cond, halo, flux, fluxhalo, out, s0, s1, cx):
    below = halo[0].astype(F32).reshape(32, 8, 256)
    above = halo[1].astype(F32).reshape(32, 8, 256)
    s0[...] = jnp.concatenate([solid[...], above[:, 0:4], below[:, 0:4]], axis=1)
    cx[...] = CONDUCT_RATE * jnp.concatenate([cond[...], above[:, 4:8], below[:, 4:8]], axis=1)
    wide = jnp.concatenate([flux[...], fluxhalo[1], fluxhalo[0]], axis=0)
    src, dst = s0, s1
    for step in range(SUBCYCLES):
        for z in range(32):
            centre = src[z]
            zbelow = src[max(z - 1, 0)]
            zabove = src[z + 1] if z < 31 else jnp.zeros_like(centre)
            spread = zbelow + zabove + pltpu.roll(centre, 1, 0) + pltpu.roll(centre, 23, 0)
            spread = spread + pltpu.roll(centre, 1, 1) + pltpu.roll(centre, 255, 1) - 6.0 * centre
            value = centre + cx[z] * spread
            if z == 0:
                value = value + wide
            if step == SUBCYCLES - 1:
                out[z] = value[0:16]
            else:
                dst[z] = value
        src, dst = dst, src


def solid_steps(solid, cond, halo, flux, fluxhalo):
    return pl.pallas_call(
        solid_kernel,
        out_shape=jax.ShapeDtypeStruct((32, 16, 256), F32),
        in_specs=[VMEM] * 5,
        out_specs=VMEM,
        scratch_shapes=[pltpu.VMEM((32, 24, 256), F32)] * 3,
        compiler_params=params(),
        name="solid",
    )(solid, cond, halo, flux, fluxhalo)


def body(flow, vel, heat, solid, cond, table, fp, sd, sp, b):
    fp, sd, sp, b = (v.reshape(1, NK) for v in (fp, sd, sp, b))
    fe, se, wall_edge, rank, ids = prep(flow, solid, cond, sd, sp)
    ag, idr, fh, sh = first_exchange(wall_edge, ids, fe, se)
    wk, wall = forward(table.reshape(256, 1024), ag, b, fp, sd, sp)
    pred, pe = predictor(flow, fh, wall, vel, heat)
    ph = pair_exchange(pe, 1)
    flow_out, flux = corrector(pred, ph, wall, vel, heat, flow)
    zr = slots_exchange(backward(flux, wk, fp, sd, rank))
    edges, face = gather_up(zr, idr)
    facehalo = pair_exchange(edges, 2)
    return flow_out, solid_steps(solid, cond, sh, face, facehalo)


def solution(mesh):
    placed = (
        P(None, ("grp", "dom"), None),
        P(None, None, ("grp", "dom"), None),
        P(None, ("grp", "dom"), None),
        P(None, ("grp", "dom"), None),
        P(None, ("grp", "dom"), None),
        P(),
        P(("grp", "dom")),
        P(("grp", "dom"), None),
        P(("grp", "dom")),
        P(("grp", "dom")),
    )
    return jax.shard_map(
        body,
        mesh=mesh,
        in_specs=placed,
        out_specs=(P(None, ("grp", "dom"), None), P(None, ("grp", "dom"), None)),
        check_vma=False,
    )
```

```python
import jax
import jax.numpy as jnp
from jax import lax
from jax.experimental import pallas as pl
from jax.experimental.pallas import tpu as pltpu
from jax.sharding import PartitionSpec as P

MESH = pl.DeviceIdType.MESH
F32, BF16, I32, I16 = jnp.float32, jnp.bfloat16, jnp.int32, jnp.int16

SUBCYCLES = 4
DIFFUSION = 0.8
TIMESTEP = 0.12
FILM_COEFF = 1.0
CONDUCT_RATE = 0.08
FLUX_GAIN = 0.25

DEV = 128
KT = 256
NK = 4096
TILES = NK // KT
ZB = 16
NN = (((1,), (0,)), ((), ()))
NT = (((1,), (1,)), ((), ()))


def dot(a, b, dims=NN):
    return lax.dot_general(a, b, dims, preferred_element_type=F32)


def narrow(row):
    return jnp.broadcast_to(row, (16, row.shape[1])).astype(I16)


def onehot(row, rows):
    key = narrow(row)
    place = lax.broadcasted_iota(I32, key.shape, 0).astype(I16)
    one, zero = BF16(1), BF16(0)
    return jnp.concatenate(
        [jnp.where(place == key - I16(16 * v), one, zero) for v in range(rows // 16)], axis=0
    )


def spread(key, count, value):
    key = narrow(key)
    return jnp.concatenate([jnp.where(key == I16(v), value, BF16(0)) for v in range(count)], axis=0)


def choose(key, count, blocks):
    key = jnp.broadcast_to(key, (8, key.shape[1]))
    low = high = jnp.zeros(key.shape, F32)
    for v in range(count):
        mask = key == v
        low = jnp.where(mask, blocks[v * 16 : v * 16 + 8], low)
        high = jnp.where(mask, blocks[v * 16 + 8 : v * 16 + 16], high)
    return low, high


def split(value):
    high = value.astype(BF16)
    return high, (value - high.astype(F32)).astype(BF16)


def beside(value):
    high, low = split(value.T)
    return jnp.concatenate([high, low], axis=1)


def swap_halves(low, high):
    axis = low.ndim - 1
    left = lax.broadcasted_iota(I32, low.shape, axis) < 64
    return jnp.where(left, low, pltpu.roll(high, 64, axis)), jnp.where(
        left, pltpu.roll(low, 64, axis), high
    )


def tile_at(t, size=KT):
    return pl.ds(pl.multiple_of(t * size, size), size)


def coords(device):
    return (device // 64, device % 64)


def remote(src, dst, send, recv, device):
    return pltpu.make_async_remote_copy(
        src_ref=src,
        dst_ref=dst,
        send_sem=send,
        recv_sem=recv,
        device_id=coords(device),
        device_id_type=MESH,
    )


def pair_copies(me, edges, halo, sems):
    up = remote(edges.at[1], halo.at[0], sems.at[0], sems.at[1], (me + 1) % DEV)
    down = remote(edges.at[0], halo.at[1], sems.at[2], sems.at[3], (me + DEV - 1) % DEV)
    return up, down


def start_all(copies):
    for copy in copies:
        copy.start()


def wait_all(copies):
    for copy in copies:
        copy.wait()


def scatter_start(me, src, dst, sems):
    @pl.loop(1, DEV)
    def _(o):
        to = (me + o) % DEV
        remote(src.at[to], dst.at[me], sems.at[0], sems.at[1], to).start()

    dst[me] = src[me]


def scatter_wait(ref, sems, which):
    many = ref.at[pl.ds(0, DEV - 1)]
    pltpu.make_async_copy(many, many, sems.at[which]).wait()


def rank_and_ids(sd_ref, sp_ref, rank, ids, carry, acc):
    before = lax.broadcasted_iota(I32, (KT, KT), 0) < lax.broadcasted_iota(I32, (KT, KT), 1)
    before = jnp.where(before, 1.0, 0.0).astype(BF16)
    every = jnp.ones((KT, KT), BF16)
    carry[...] = jnp.zeros_like(carry)
    acc[...] = jnp.zeros_like(acc)

    @pl.loop(0, TILES)
    def _(t):
        k = tile_at(t)
        sd = sd_ref[:, k]
        mine = lax.broadcasted_iota(I32, (DEV, KT), 0) == sd
        one = onehot(sd, DEV)
        ahead = dot(one, before) + carry[...]
        r = jnp.sum(jnp.where(mine, ahead, 0.0), axis=0, keepdims=True).astype(I32)
        carry[...] += dot(one, every)
        rank[:, k] = r
        tag = (sp_ref[:, k] + 1).astype(F32)
        place = lax.broadcasted_iota(I32, (32, KT), 0)
        m = jnp.where(place == sd % 32, tag, 0.0).astype(BF16)
        acc[...] += dot(m, onehot((sd // 32) * 64 + r, 256), NT)

    got = acc[...]
    left = lax.broadcasted_iota(I32, (32, 128), 1) < 64
    for t in range(2):
        both = got[:, t * 128 : (t + 1) * 128]
        turned = pltpu.roll(both, 64, 1)
        ids[t * 64 : t * 64 + 32] = jnp.where(left, both, turned).reshape(32, 1, 128)
        ids[t * 64 + 32 : t * 64 + 64] = jnp.where(left, turned, both).reshape(32, 1, 128)


def flow_edges(field, edges):
    @pl.loop(0, 128 // ZB)
    def _(b):
        z0 = pl.multiple_of(b * ZB, ZB)
        block = field[pl.ds(z0 + 1, ZB)]
        edges[0, pl.ds(z0, ZB), :] = block[:, 0, :].astype(BF16)
        edges[1, pl.ds(z0, ZB), :] = block[:, 15, :].astype(BF16)


def solid_edges(solid, cond, edges):
    low = jnp.concatenate([solid[:, 0:4, :], cond[:, 0:4, :]], axis=1)
    high = jnp.concatenate([solid[:, 12:16, :], cond[:, 12:16, :]], axis=1)
    edges[0] = low.reshape(16, 16, 256).astype(BF16)
    edges[1] = high.reshape(16, 16, 256).astype(BF16)


def pick_tags(idr, s):
    left = lax.broadcasted_iota(I32, (1, 128), 1) < 64
    pairs = [jnp.where(left, idr[s + 2 * p], idr[s + 2 * p + 1]) for p in range(2)]
    return jnp.concatenate(pairs, axis=1).astype(I32) - 1


def answers(idr, solid, xs, wl):
    wl[...] = beside(solid[0])

    @pl.loop(0, DEV // 4)
    def _(t):
        tag = pick_tags(idr, t * 4)
        row = onehot(tag >> 4, 16)
        blocks = dot(wl[...], jnp.concatenate([row, row], axis=0))
        low, high = choose(tag & 15, 16, blocks)
        for p in range(2):
            lanes = slice(p * 128, (p + 1) * 128)
            one, two = swap_halves(low[:, lanes], high[:, lanes])
            xs[t * 4 + 2 * p] = one
            xs[t * 4 + 2 * p + 1] = two


def weights(tab, b_ref, wk, first, last):
    @pl.loop(first, last)
    def _(t):
        k = tile_at(t)
        block = onehot(b_ref[:, k], 1024)
        wk[:, k] = dot(tab[0], block) + dot(tab[1], block)


def forward(xr, fp_ref, sd_ref, rank, wk, lhs, acc, face):
    for t in range(2):
        d = t * 64
        low, high = swap_halves(xr[d : d + 32], xr[d + 32 : d + 64])
        both = jnp.concatenate([low, high], axis=1).reshape(512, 128)
        lhs[0, :, t * 128 : (t + 1) * 128], lhs[1, :, t * 128 : (t + 1) * 128] = split(both)
    acc[...] = jnp.zeros_like(acc)

    @pl.loop(0, TILES)
    def _(t):
        k = tile_at(t)
        fp, sd, r = fp_ref[:, k], sd_ref[:, k], rank[:, k]
        slot = onehot((sd >> 5) * 64 + r, 256)
        blocks = dot(lhs[0], slot) + dot(lhs[1], slot)
        low, high = choose(sd & 31, 32, blocks)
        w = wk[:, k]
        y = jnp.concatenate(
            [
                jnp.sum(
                    w[i * 16 : i * 16 + 8] * low + w[i * 16 + 8 : i * 16 + 16] * high,
                    axis=0,
                    keepdims=True,
                )
                for i in range(16)
            ],
            axis=0,
        )
        yhigh, ylow = split(y)
        row = onehot(fp >> 4, 16)
        col = fp & 15
        acc[...] += dot(spread(col, 16, yhigh), row, NT) + dot(spread(col, 16, ylow), row, NT)

    face[...] = acc[...].T


def backward(flux, wk, fp_ref, sd_ref, rank, fl, acc, z):
    fl[...] = beside(flux)
    acc[...] = jnp.zeros_like(acc)

    @pl.loop(0, TILES)
    def _(t):
        k = tile_at(t)
        fp, sd, r = fp_ref[:, k], sd_ref[:, k], rank[:, k]
        row = onehot(fp >> 4, 16)
        low, high = choose(fp & 15, 16, dot(fl[...], jnp.concatenate([row, row], axis=0)))
        value = jnp.zeros((16, KT), F32)
        for i in range(16):
            y = low[i : i + 1] if i < 8 else high[i - 8 : i - 7]
            value = value + wk[i * 16 : (i + 1) * 16, k] * y
        vhigh, vlow = split(value)
        slot = onehot((sd >> 5) * 64 + r, 256)
        e = sd & 31
        acc[...] += dot(spread(e, 32, vhigh), slot, NT) + dot(spread(e, 32, vlow), slot, NT)

    got = acc[...]
    for t in range(2):
        both = got[:, t * 128 : (t + 1) * 128].reshape(32, 16, 128)
        d = t * 64
        z[d : d + 32], z[d + 32 : d + 64] = swap_halves(both[:, 0:8], both[:, 8:16])


def gather_up(zr, idr, acc):
    acc[...] = jnp.zeros_like(acc)

    @pl.loop(0, DEV // 4)
    def _(t):
        tag = pick_tags(idr, t * 4)
        lows, highs = [], []
        for p in range(2):
            low, high = swap_halves(zr[t * 4 + 2 * p], zr[t * 4 + 2 * p + 1])
            lows.append(low)
            highs.append(high)
        value = jnp.concatenate(
            [jnp.concatenate(lows, axis=1), jnp.concatenate(highs, axis=1)], axis=0
        )
        vhigh, vlow = split(value)
        row = onehot(tag >> 4, 16)
        col = tag & 15
        acc[...] += dot(spread(col, 16, vhigh), row, NT) + dot(spread(col, 16, vlow), row, NT)

    return acc[...].T * FLUX_GAIN


def slope_of(field, index, xlow, xhigh, vel, heat, z):
    centre = field[index]
    rows = lax.broadcasted_iota(I32, (16, 256), 0)
    xbelow = jnp.where(rows == 0, xlow, pltpu.roll(centre, 1, 0))
    xabove = jnp.where(rows == 15, xhigh, pltpu.roll(centre, 15, 0))
    sides = (
        (field[index - 1], field[index + 1]),
        (xbelow, xabove),
        (pltpu.roll(centre, 1, 1), pltpu.roll(centre, 255, 1)),
    )
    total = heat[z].astype(F32)
    for axis, (below, above) in enumerate(sides):
        c = vel[axis, z].astype(F32)
        weight = jnp.maximum(c, 0.0) + DIFFUSION
        total = total + (below - centre) * weight + (above - centre) * (weight - c)
    return centre, total


def predict_block(field, halo, vel, heat, pred, edges, z0, count):
    xlow = halo[0, pl.ds(z0, ZB), :].astype(F32)
    xhigh = halo[1, pl.ds(z0, ZB), :].astype(F32)
    first, last = [], []
    for q in range(count):
        z = z0 + q
        centre, slope = slope_of(
            field, z + 1, xlow[q : q + 1], xhigh[q : q + 1], vel, heat, z
        )
        value = centre + TIMESTEP * slope
        pred[z + 1] = value
        first.append(value[0:1])
        last.append(value[15:16])
    for _ in range(count, ZB):
        first.append(jnp.zeros((1, 256), F32))
        last.append(jnp.zeros((1, 256), F32))
    edges[0, pl.ds(z0, ZB), :] = jnp.concatenate(first, axis=0).astype(BF16)
    edges[1, pl.ds(z0, ZB), :] = jnp.concatenate(last, axis=0).astype(BF16)


def correct_block(pred, halo, vel, heat, field, z0, count):
    xlow = halo[0, pl.ds(z0, ZB), :].astype(F32)
    xhigh = halo[1, pl.ds(z0, ZB), :].astype(F32)
    for q in range(count):
        z = z0 + q
        centre, slope = slope_of(pred, z + 1, xlow[q : q + 1], xhigh[q : q + 1], vel, heat, z)
        field[z + 1] = 0.5 * field[z + 1] + 0.5 * (centre + TIMESTEP * slope)


def widen(own, above, below):
    return jnp.concatenate([own, above, below], axis=own.ndim - 2)


def spread_of(src, z, layers):
    centre = src[z]
    zbelow = src[max(z - 1, 0)]
    zabove = src[z + 1] if z + 1 < layers else jnp.zeros_like(centre)
    total = zbelow + zabove + pltpu.roll(centre, 1, 0) + pltpu.roll(centre, 23, 0)
    return centre, total + pltpu.roll(centre, 1, 1) + pltpu.roll(centre, 255, 1) - 6.0 * centre


def solid_base(solid, cond, halo, s0, s1, cx):
    below = halo[0].astype(F32).reshape(32, 8, 256)
    above = halo[1].astype(F32).reshape(32, 8, 256)
    s0[...] = widen(solid[...], above[:, 0:4], below[:, 0:4])
    cx[...] = CONDUCT_RATE * widen(cond[...], above[:, 4:8], below[:, 4:8])
    src, dst = s0, s1
    for step in range(SUBCYCLES):
        for z in range(32):
            centre, total = spread_of(src, z, 32)
            dst[z] = centre + cx[z] * total
        src, dst = dst, src


def flux_response(wide, cx, t0, t1):
    t0[...] = jnp.zeros_like(t0)
    t1[...] = jnp.zeros_like(t1)
    t0[0] = wide
    src, dst = t0, t1
    for step in range(1, SUBCYCLES):
        for z in range(step + 1):
            centre, total = spread_of(src, z, 5)
            value = centre + cx[z] * total
            dst[z] = value + wide if z == 0 else value
        src, dst = dst, src
    return src


def kernel(
    flow_in, vel_in, heat_in, solid_in, cond_in, table_in, fp, sd, sp, b,
    flow_out, solid_out,
    field, pred, vel, heat, solid, cond, table, tab, wk, wall, wallt,
    rank, ids, idr, xs, xr, z, zr, lhs, wl,
    fe, fh, pe, ph, pt, pth, se, sh, ff, ffh,
    s0, s1, cx, t0, t1, carry, idacc, acc, zacc,
    insem, outsem, isem, xsem, zsem, psem,
):
    me = lax.axis_index("grp") * 64 + lax.axis_index("dom")
    barrier = pltpu.get_barrier_semaphore()

    loads = [
        pltpu.make_async_copy(src, dst, insem.at[i])
        for i, (src, dst) in enumerate(
            (
                (solid_in, solid),
                (cond_in, cond),
                (flow_in, field.at[pl.ds(1, 128)]),
                (table_in, table),
                (vel_in, vel),
                (heat_in, heat),
            )
        )
    ]
    start_all(loads)

    @pl.loop(1, DEV)
    def _(o):
        pl.semaphore_signal(barrier, inc=1, device_id=coords((me + o) % DEV), device_id_type=MESH)

    rank_and_ids(sd, sp, rank, ids, carry, idacc)
    loads[0].wait()
    loads[1].wait()
    solid_edges(solid, cond, se)
    loads[2].wait()
    zero = jnp.zeros((16, 256), F32)
    field[0] = zero
    field[129] = zero
    pred[0] = zero
    flow_edges(field, fe)

    pl.semaphore_wait(barrier, DEV - 1)
    scatter_start(me, ids, idr, isem)
    flow_halo = pair_copies(me, fe, fh, psem.at[0])
    solid_halo = pair_copies(me, se, sh, psem.at[1])
    start_all(flow_halo + solid_halo)

    loads[3].wait()
    tab[0], tab[1] = split(table[...])
    weights(tab, b, wk, 0, W_FIRST)

    scatter_wait(idr, isem, 1)
    answers(idr, solid, xs, wl)
    scatter_start(me, xs, xr, xsem)

    weights(tab, b, wk, W_FIRST, TILES)
    loads[4].wait()
    loads[5].wait()
    wait_all(flow_halo)

    @pl.loop(0, 128 // ZB - 1)
    def _(n):
        predict_block(field, fh, vel, heat, pred, pe, pl.multiple_of(n * ZB, ZB), ZB)

    predict_block(field, fh, vel, heat, pred, pe, 128 - ZB, ZB - 1)
    pred_halo = pair_copies(me, pe, ph, psem.at[2])
    start_all(pred_halo)

    scatter_wait(xr, xsem, 1)
    forward(xr, fp, sd, rank, wk, lhs, acc, wall)

    field[129] = wall[...]
    pred[129] = wall[...]
    xlow = fh[0, 112:128, :].astype(F32)[15:16]
    xhigh = fh[1, 112:128, :].astype(F32)[15:16]
    centre, slope = slope_of(field, 128, xlow, xhigh, vel, heat, 127)
    top = centre + TIMESTEP * slope
    pred[128] = top
    pt[0] = top[0:1]
    pt[1] = top[15:16]
    top_halo = pair_copies(me, pt, pth, psem.at[3])
    start_all(top_halo)

    wait_all(pred_halo)

    def correct(n):
        z0 = pl.multiple_of(n * ZB, ZB)
        correct_block(pred, ph, vel, heat, field, z0, ZB)
        out = pl.ds(z0, ZB)
        pltpu.make_async_copy(field.at[pl.ds(z0 + 1, ZB)], flow_out.at[out], outsem.at[n]).start()

    @pl.loop(0, C_FIRST)
    def _(n):
        correct(n)

    wait_all(top_halo)
    centre, slope = slope_of(pred, 128, pth[0], pth[1], vel, heat, 127)
    done = 0.5 * field[128] + 0.5 * (centre + TIMESTEP * slope)
    field[128] = done
    flux = FILM_COEFF * (done - wall[...])
    backward(flux, wk, fp, sd, rank, wl, zacc, z)
    scatter_start(me, z, zr, zsem)

    @pl.loop(C_FIRST, 128 // ZB - 1)
    def _(n):
        correct(n)

    correct_block(pred, ph, vel, heat, field, 128 - ZB, ZB - 1)
    last = 128 // ZB - 1
    pltpu.make_async_copy(
        field.at[pl.ds(129 - ZB, ZB)], flow_out.at[pl.ds(128 - ZB, ZB)], outsem.at[last]
    ).start()
    wait_all(solid_halo)
    solid_base(solid, cond, sh, s0, s1, cx)
    rest = pltpu.make_async_copy(
        s0.at[pl.ds(4, 28), pl.ds(0, 16)], solid_out.at[pl.ds(4, 28)], outsem.at[8]
    )
    rest.start()

    scatter_wait(zr, zsem, 1)
    total = gather_up(zr, idr, acc)
    ff[0] = total[0:4]
    ff[1] = total[12:16]
    face_halo = pair_copies(me, ff, ffh, psem.at[4])
    start_all(face_halo)
    wait_all(face_halo)
    response = flux_response(widen(total, ffh[1], ffh[0]), cx, t0, t1)
    solid[0:4] = s0[0:4, 0:16, :] + response[0:4, 0:16, :]
    near = pltpu.make_async_copy(solid.at[pl.ds(0, 4)], solid_out.at[pl.ds(0, 4)], outsem.at[9])
    near.start()

    @pl.loop(0, 128 // ZB)
    def _(n):
        out = pl.ds(pl.multiple_of(n * ZB, ZB), ZB)
        pltpu.make_async_copy(field.at[pl.ds(n * ZB + 1, ZB)], flow_out.at[out], outsem.at[n]).wait()

    scatter_wait(ids, isem, 0)
    scatter_wait(xs, xsem, 0)
    scatter_wait(z, zsem, 0)
    rest.wait()
    near.wait()


W_FIRST = 8
C_FIRST = 2


def body(flow, vel, heat, solid, cond, table, fp, sd, sp, b):
    fp, sd, sp, b = (v.reshape(1, NK) for v in (fp, sd, sp, b))
    vm, hbm = pl.BlockSpec(memory_space=pltpu.VMEM), pl.BlockSpec(memory_space=pl.ANY)
    dma = pltpu.SemaphoreType.DMA
    scratch = [
        pltpu.VMEM((130, 16, 256), F32),
        pltpu.VMEM((130, 16, 256), F32),
        pltpu.VMEM((3, 128, 16, 256), BF16),
        pltpu.VMEM((128, 16, 256), BF16),
        pltpu.VMEM((32, 16, 256), F32),
        pltpu.VMEM((32, 16, 256), F32),
        pltpu.VMEM((256, 1024), F32),
        pltpu.VMEM((2, 256, 1024), BF16),
        pltpu.VMEM((256, NK), F32),
        pltpu.VMEM((16, 256), F32),
        pltpu.VMEM((16, 256), F32),
        pltpu.VMEM((1, NK), I32),
        pltpu.VMEM((DEV, 1, 128), F32),
        pltpu.VMEM((DEV, 1, 128), F32),
        pltpu.VMEM((DEV, 8, 128), F32),
        pltpu.VMEM((DEV, 8, 128), F32),
        pltpu.VMEM((DEV, 8, 128), F32),
        pltpu.VMEM((DEV, 8, 128), F32),
        pltpu.VMEM((2, 512, 256), BF16),
        pltpu.VMEM((256, 32), BF16),
        pltpu.VMEM((2, 128, 256), BF16),
        pltpu.VMEM((2, 128, 256), BF16),
        pltpu.VMEM((2, 128, 256), BF16),
        pltpu.VMEM((2, 128, 256), BF16),
        pltpu.VMEM((2, 1, 256), F32),
        pltpu.VMEM((2, 1, 256), F32),
        pltpu.VMEM((2, 16, 16, 256), BF16),
        pltpu.VMEM((2, 16, 16, 256), BF16),
        pltpu.VMEM((2, 4, 256), F32),
        pltpu.VMEM((2, 4, 256), F32),
        pltpu.VMEM((32, 24, 256), F32),
        pltpu.VMEM((32, 24, 256), F32),
        pltpu.VMEM((32, 24, 256), F32),
        pltpu.VMEM((5, 24, 256), F32),
        pltpu.VMEM((5, 24, 256), F32),
        pltpu.VMEM((DEV, KT), F32),
        pltpu.VMEM((32, 256), F32),
        pltpu.VMEM((256, 16), F32),
        pltpu.VMEM((512, 256), F32),
        dma((6,)),
        dma((10,)),
        dma((2,)),
        dma((2,)),
        dma((2,)),
        dma((5, 4)),
    ]
    return pl.pallas_call(
        kernel,
        out_shape=(
            jax.ShapeDtypeStruct((128, 16, 256), F32),
            jax.ShapeDtypeStruct((32, 16, 256), F32),
        ),
        in_specs=[hbm] * 6 + [vm] * 4,
        out_specs=(hbm, hbm),
        scratch_shapes=scratch,
        compiler_params=pltpu.CompilerParams(
            vmem_limit_bytes=60 * 1024 * 1024, collective_id=0, has_side_effects=True
        ),
        name="coupled",
    )(flow, vel, heat, solid, cond, table.reshape(256, 1024), fp, sd, sp, b)


def solution(mesh):
    placed = (
        P(None, ("grp", "dom"), None),
        P(None, None, ("grp", "dom"), None),
        P(None, ("grp", "dom"), None),
        P(None, ("grp", "dom"), None),
        P(None, ("grp", "dom"), None),
        P(),
        P(("grp", "dom")),
        P(("grp", "dom"), None),
        P(("grp", "dom")),
        P(("grp", "dom")),
    )
    return jax.shard_map(
        body,
        mesh=mesh,
        in_specs=placed,
        out_specs=(P(None, ("grp", "dom"), None), P(None, ("grp", "dom"), None)),
        check_vma=False,
    )
```

```python
import jax
import jax.numpy as jnp
from jax import lax
from jax.experimental import pallas as pl
from jax.experimental.pallas import tpu as pltpu
from jax.sharding import PartitionSpec as P

MESH = pl.DeviceIdType.MESH
F32, BF16, I32, I16 = jnp.float32, jnp.bfloat16, jnp.int32, jnp.int16

SUBCYCLES = 4
DIFFUSION = 0.8
TIMESTEP = 0.12
FILM_COEFF = 1.0
CONDUCT_RATE = 0.08
FLUX_GAIN = 0.25

DEV = 128
KT = 256
NK = 4096
TILES = NK // KT
ZB = 16
NN = (((1,), (0,)), ((), ()))
NT = (((1,), (1,)), ((), ()))


def dot(a, b, dims=NN):
    return lax.dot_general(a, b, dims, preferred_element_type=F32)


def narrow(row):
    return jnp.broadcast_to(row, (16, row.shape[1])).astype(I16)


def onehot(row, rows):
    key = narrow(row)
    place = lax.broadcasted_iota(I32, key.shape, 0).astype(I16)
    one, zero = BF16(1), BF16(0)
    return jnp.concatenate(
        [jnp.where(place == key - I16(16 * v), one, zero) for v in range(rows // 16)], axis=0
    )


def spread(key, count, value):
    key = narrow(key)
    return jnp.concatenate([jnp.where(key == I16(v), value, BF16(0)) for v in range(count)], axis=0)


def choose(key, count, blocks):
    key = jnp.broadcast_to(key, (8, key.shape[1]))
    low = high = jnp.zeros(key.shape, F32)
    for v in range(count):
        mask = key == v
        low = jnp.where(mask, blocks[v * 16 : v * 16 + 8], low)
        high = jnp.where(mask, blocks[v * 16 + 8 : v * 16 + 16], high)
    return low, high


def split(value):
    high = value.astype(BF16)
    return high, (value - high.astype(F32)).astype(BF16)


def beside(value):
    high, low = split(value.T)
    return jnp.concatenate([high, low], axis=1)


def swap_halves(low, high):
    axis = low.ndim - 1
    left = lax.broadcasted_iota(I32, low.shape, axis) < 64
    return jnp.where(left, low, pltpu.roll(high, 64, axis)), jnp.where(
        left, pltpu.roll(low, 64, axis), high
    )


def encode(value):
    step = jnp.floor(jnp.clip(value * CODE, -32767.0, 32767.0) + 0.5)
    return step.astype(I32).astype(I16)


def tile_at(t, size=KT):
    return pl.ds(pl.multiple_of(t * size, size), size)


def coords(device):
    return (lax.div(device, 64), lax.rem(device, 64))


def peer(me, offset):
    return lax.rem(me + offset, DEV)


def remote(src, dst, send, recv, device):
    return pltpu.make_async_remote_copy(
        src_ref=src,
        dst_ref=dst,
        send_sem=send,
        recv_sem=recv,
        device_id=coords(device),
        device_id_type=MESH,
    )


def pair_copies(me, edges, halo, sems):
    up = remote(edges.at[1], halo.at[0], sems.at[0], sems.at[1], peer(me, 1))
    down = remote(edges.at[0], halo.at[1], sems.at[2], sems.at[3], peer(me, DEV - 1))
    return up, down


def start_all(copies):
    for copy in copies:
        copy.start()


def wait_all(copies):
    for copy in copies:
        copy.wait()


def scatter_one(me, to, src, dst, sems):
    remote(src.at[to], dst.at[me], sems.at[0], sems.at[1], to).start()


def scatter_start(me, src, dst, sems):
    for o in range(1, 8):
        scatter_one(me, peer(me, o), src, dst, sems)

    @pl.loop(1, DEV // 8)
    def _(n):
        for q in range(8):
            scatter_one(me, peer(me, n * 8 + q), src, dst, sems)

    dst[me] = src[me]


def scatter_wait(ref, sems, which):
    many = ref.at[pl.ds(0, DEV - 1)]
    pltpu.make_async_copy(many, many, sems.at[which]).wait()


def rank_and_ids(sd_ref, sp_ref, rank, ids, carry, acc, beside_it):
    before = lax.broadcasted_iota(I32, (KT, KT), 0) < lax.broadcasted_iota(I32, (KT, KT), 1)
    before = jnp.where(before, 1.0, 0.0).astype(BF16)
    every = jnp.ones((KT, KT), BF16)
    carry[...] = jnp.zeros_like(carry)
    acc[...] = jnp.zeros_like(acc)

    @pl.loop(0, TILES // 4)
    def _(n):
        beside_it(n)
        held, total = carry[...], jnp.zeros((32, 256), F32)
        for u in range(4):
            k = tile_at(n * 4 + u)
            sd = sd_ref[:, k]
            mine = lax.broadcasted_iota(I32, (DEV, KT), 0) == sd
            one = onehot(sd, DEV)
            ahead = dot(one, before) + held
            r = jnp.sum(jnp.where(mine, ahead, 0.0), axis=0, keepdims=True).astype(I32)
            held = held + dot(one, every)
            rank[:, k] = r
            tag = (sp_ref[:, k] + 1).astype(F32)
            place = lax.broadcasted_iota(I32, (32, KT), 0)
            m = jnp.where(place == (sd & 31), tag, 0.0).astype(BF16)
            total = total + dot(m, onehot((sd >> 5) * 64 + r, 256), NT)
        carry[...] = held
        acc[...] += total

    got = acc[...]
    left = lax.broadcasted_iota(I32, (32, 128), 1) < 64
    for t in range(2):
        both = got[:, t * 128 : (t + 1) * 128]
        turned = pltpu.roll(both, 64, 1)
        ids[t * 64 : t * 64 + 32] = jnp.where(left, both, turned).reshape(32, 1, 128)
        ids[t * 64 + 32 : t * 64 + 64] = jnp.where(left, turned, both).reshape(32, 1, 128)


def flow_edges(field, edges):
    @pl.loop(0, 128 // ZB)
    def _(b):
        z0 = pl.multiple_of(b * ZB, ZB)
        block = field[pl.ds(z0 + 1, ZB)]
        edges[0, pl.ds(z0, ZB), :] = block[:, 0, :].astype(BF16)
        edges[1, pl.ds(z0, ZB), :] = block[:, 15, :].astype(BF16)


def solid_edges(solid, cond, edges):
    low = jnp.concatenate([solid[:, 0:4, :], cond[:, 0:4, :]], axis=1)
    high = jnp.concatenate([solid[:, 12:16, :], cond[:, 12:16, :]], axis=1)
    edges[0] = low.reshape(16, 16, 256).astype(BF16)
    edges[1] = high.reshape(16, 16, 256).astype(BF16)


def pick_tags(idr, s):
    left = lax.broadcasted_iota(I32, (1, 128), 1) < 64
    pairs = [jnp.where(left, idr[s + 2 * p], idr[s + 2 * p + 1]) for p in range(2)]
    return jnp.concatenate(pairs, axis=1).astype(I32) - 1


def answers(me, idr, solid, xs, xr, wl, sems):
    wl[...] = beside(solid[0])
    first, turn = lax.div(me, 16), lax.rem(me, 16)

    def send(n):
        base = lax.rem(first + n, 8) * 16

        @pl.loop(0, 16)
        def _(q):
            to = base + lax.rem(turn + q, 16)

            @pl.when(to != me)
            def _():
                scatter_one(me, to, xs, xr, sems)

    @pl.loop(0, 8)
    def _(n):
        @pl.when(n > 0)
        def _():
            send(n + 7)

        base = lax.rem(first + n, 8) * 16
        for u in range(4):
            s = base + u * 4
            tag = pick_tags(idr, s)
            row = onehot(tag >> 4, 16)
            blocks = dot(wl[...], jnp.concatenate([row, row], axis=0))
            low, high = choose(tag & 15, 16, blocks)
            for p in range(2):
                lanes = slice(p * 128, (p + 1) * 128)
                one, two = swap_halves(low[:, lanes], high[:, lanes])
                xs[s + 2 * p] = encode(one)
                xs[s + 2 * p + 1] = encode(two)

    send(7)
    xr[me] = xs[me]


def weights(tab, b_ref, wk):
    @pl.loop(0, TILES)
    def _(t):
        k = tile_at(t)
        block = onehot(b_ref[:, k], 1024)
        wk[:, k] = dot(tab[0], block) + dot(tab[1], block)


def forward(xr, fp_ref, sd_ref, rank, wk, lhs, acc, face):
    for t in range(2):
        d = t * 64
        one = xr[d : d + 32].astype(I32).astype(F32)
        two = xr[d + 32 : d + 64].astype(I32).astype(F32)
        both = jnp.concatenate(swap_halves(one, two), axis=1).reshape(512, 128)
        high, low = split(both)
        lhs[:, t * 128 : (t + 1) * 128] = high
        lhs[:, 256 + t * 128 : 256 + (t + 1) * 128] = low
    acc[...] = jnp.zeros_like(acc)

    @pl.loop(0, TILES // FU)
    def _(n):
        spreads, rows = [], []
        for u in range(FU):
            k = tile_at(n * FU + u)
            fp, sd, r = fp_ref[:, k], sd_ref[:, k], rank[:, k]
            slot = onehot((sd >> 5) * 64 + r, 256)
            blocks = dot(lhs[...], jnp.concatenate([slot, slot], axis=0))
            low, high = choose(sd & 31, 32, blocks)
            w = wk[:, k]
            y = jnp.concatenate(
                [
                    jnp.sum(
                        w[i * 16 : i * 16 + 8] * low + w[i * 16 + 8 : i * 16 + 16] * high,
                        axis=0,
                        keepdims=True,
                    )
                    for i in range(16)
                ],
                axis=0,
            )
            row = onehot(fp >> 4, 16)
            for part in split(y * (1.0 / CODE)):
                spreads.append(spread(fp & 15, 16, part))
                rows.append(row)
        acc[...] += dot(jnp.concatenate(spreads, axis=1), jnp.concatenate(rows, axis=1), NT)

    face[...] = acc[...].T


def backward(me, flux, wk, fp_ref, sd_ref, rank, fl, vs, acc, z, zr, sems):
    fl[...] = beside(flux)

    @pl.loop(0, TILES // BU)
    def _(n):
        for u in range(BU):
            k = tile_at(n * BU + u)
            fp = fp_ref[:, k]
            row = onehot(fp >> 4, 16)
            low, high = choose(fp & 15, 16, dot(fl[...], jnp.concatenate([row, row], axis=0)))
            value = jnp.zeros((16, KT), F32)
            for i in range(16):
                y = low[i : i + 1] if i < 8 else high[i - 8 : i - 7]
                value = value + wk[i * 16 : (i + 1) * 16, k] * y
            vs[0, :, k], vs[1, :, k] = split(value)

    turn = lax.rem(me, 64)

    def send(half, i):
        j = lax.rem(turn + i, 64)
        to = lax.div(j, 16) * 32 + half * 16 + lax.rem(j, 16)

        @pl.when(to != me)
        def _():
            scatter_one(me, to, z, zr, sems)

    for half in range(2):
        acc[...] = jnp.zeros_like(acc)

        @pl.loop(0, TILES // 4)
        def _(n):
            if half:
                for i in range(16):
                    send(0, n * 16 + i)
            spreads, slots = [], []
            for u in range(4):
                k = tile_at(n * 4 + u)
                sd, r = sd_ref[:, k], rank[:, k]
                slot = onehot((sd >> 5) * 64 + r, 256)
                e = (sd & 31) - half * 16
                for part in range(2):
                    spreads.append(spread(e, 16, vs[part, :, k]))
                    slots.append(slot)
            acc[...] += dot(jnp.concatenate(spreads, axis=1), jnp.concatenate(slots, axis=1), NT)

        got = acc[...]
        for t in range(2):
            both = got[:, t * 128 : (t + 1) * 128].reshape(16, 16, 128)
            d = t * 64 + half * 16
            z[d : d + 16], z[d + 32 : d + 48] = swap_halves(both[:, 0:8], both[:, 8:16])

    @pl.loop(0, 16)
    def _(n):
        for i in range(4):
            send(1, n * 4 + i)

    zr[me] = z[me]


def gather_up(zr, idr, acc):
    acc[...] = jnp.zeros_like(acc)

    @pl.loop(0, DEV // 4 // GU)
    def _(n):
        spreads, rows = [], []
        for u in range(GU):
            s = (n * GU + u) * 4
            tag = pick_tags(idr, s)
            lows, highs = [], []
            for p in range(2):
                low, high = swap_halves(zr[s + 2 * p], zr[s + 2 * p + 1])
                lows.append(low)
                highs.append(high)
            value = jnp.concatenate(
                [jnp.concatenate(lows, axis=1), jnp.concatenate(highs, axis=1)], axis=0
            )
            row = onehot(tag >> 4, 16)
            for part in split(value):
                spreads.append(spread(tag & 15, 16, part))
                rows.append(row)
        acc[...] += dot(jnp.concatenate(spreads, axis=1), jnp.concatenate(rows, axis=1), NT)

    return acc[...].T * FLUX_GAIN


def slope_of(field, index, xlow, xhigh, vel, heat, z):
    centre = field[index]
    rows = lax.broadcasted_iota(I32, (16, 256), 0)
    xbelow = jnp.where(rows == 0, xlow, pltpu.roll(centre, 1, 0))
    xabove = jnp.where(rows == 15, xhigh, pltpu.roll(centre, 15, 0))
    sides = (
        (field[index - 1], field[index + 1]),
        (xbelow, xabove),
        (pltpu.roll(centre, 1, 1), pltpu.roll(centre, 255, 1)),
    )
    total = heat[z].astype(F32)
    for axis, (below, above) in enumerate(sides):
        c = vel[axis, z].astype(F32)
        weight = jnp.maximum(c, 0.0) + DIFFUSION
        total = total + (below - centre) * weight + (above - centre) * (weight - c)
    return centre, total


def predict_block(field, halo, vel, heat, pred, edges, z0, count):
    xlow = halo[0, pl.ds(z0, ZB), :].astype(F32)
    xhigh = halo[1, pl.ds(z0, ZB), :].astype(F32)
    first, last = [], []
    for q in range(count):
        z = z0 + q
        centre, slope = slope_of(
            field, z + 1, xlow[q : q + 1], xhigh[q : q + 1], vel, heat, z
        )
        value = centre + TIMESTEP * slope
        pred[z + 1] = value
        first.append(value[0:1])
        last.append(value[15:16])
    for _ in range(count, ZB):
        first.append(jnp.zeros((1, 256), F32))
        last.append(jnp.zeros((1, 256), F32))
    edges[0, pl.ds(z0, ZB), :] = jnp.concatenate(first, axis=0).astype(BF16)
    edges[1, pl.ds(z0, ZB), :] = jnp.concatenate(last, axis=0).astype(BF16)


def correct_block(pred, halo, vel, heat, field, z0, count):
    xlow = halo[0, pl.ds(z0, ZB), :].astype(F32)
    xhigh = halo[1, pl.ds(z0, ZB), :].astype(F32)
    for q in range(count):
        z = z0 + q
        centre, slope = slope_of(pred, z + 1, xlow[q : q + 1], xhigh[q : q + 1], vel, heat, z)
        field[z + 1] = 0.5 * field[z + 1] + 0.5 * (centre + TIMESTEP * slope)


def widen(own, above, below):
    return jnp.concatenate([own, above, below], axis=own.ndim - 2)


def spread_of(src, z, layers):
    centre = src[z]
    zbelow = src[max(z - 1, 0)]
    zabove = src[z + 1] if z + 1 < layers else jnp.zeros_like(centre)
    total = zbelow + zabove + pltpu.roll(centre, 1, 0) + pltpu.roll(centre, 23, 0)
    return centre, total + pltpu.roll(centre, 1, 1) + pltpu.roll(centre, 255, 1) - 6.0 * centre


def solid_base(solid, cond, halo, s0, s1, cx):
    below = halo[0].astype(F32).reshape(32, 8, 256)
    above = halo[1].astype(F32).reshape(32, 8, 256)
    s0[...] = widen(solid[...], above[:, 0:4], below[:, 0:4])
    cx[...] = CONDUCT_RATE * widen(cond[...], above[:, 4:8], below[:, 4:8])
    src, dst = s0, s1
    for step in range(SUBCYCLES):
        for z in range(32):
            centre, total = spread_of(src, z, 32)
            dst[z] = centre + cx[z] * total
        src, dst = dst, src


def flux_response(wide, cx, t0, t1):
    t0[...] = jnp.zeros_like(t0)
    t1[...] = jnp.zeros_like(t1)
    t0[0] = wide
    src, dst = t0, t1
    for step in range(1, SUBCYCLES):
        for z in range(step + 1):
            centre, total = spread_of(src, z, 5)
            value = centre + cx[z] * total
            dst[z] = value + wide if z == 0 else value
        src, dst = dst, src
    return src


def kernel(
    flow_in, vel_in, heat_in, solid_in, cond_in, table_in, fp, sd, sp, b,
    flow_out, solid_out,
    field, pred, vel, heat, solid, cond, table, tab, wk, wall, wallt,
    rank, ids, idr, xs, xr, z, zr, lhs, wl,
    fe, fh, pe, ph, pt, pth, se, sh, ff, ffh,
    s0, s1, cx, t0, t1, carry, idacc, acc, zacc, vs,
    insem, outsem, isem, xsem, zsem, psem,
):
    me = lax.axis_index("grp") * 64 + lax.axis_index("dom")
    barrier = pltpu.get_barrier_semaphore()

    loads = [
        pltpu.make_async_copy(src, dst, insem.at[i])
        for i, (src, dst) in enumerate(
            (
                (solid_in, solid),
                (cond_in, cond),
                (flow_in, field.at[pl.ds(1, 128)]),
                (table_in, table),
                (vel_in, vel),
                (heat_in, heat),
            )
        )
    ]
    start_all(loads)

    def greet(n):
        for q in range(32):
            to = peer(me, n * 32 + q)
            if q:
                pl.semaphore_signal(barrier, inc=1, device_id=coords(to), device_id_type=MESH)
            else:

                @pl.when(n > 0)
                def _():
                    pl.semaphore_signal(barrier, inc=1, device_id=coords(to), device_id_type=MESH)

    rank_and_ids(sd, sp, rank, ids, carry, idacc, greet)
    loads[3].wait()
    tab[0], tab[1] = split(table[...])
    pl.semaphore_wait(barrier, DEV - 1)

    scatter_start(me, ids, idr, isem)
    weights(tab, b, wk)
    loads[0].wait()
    loads[1].wait()
    solid_edges(solid, cond, se)
    loads[2].wait()
    zero = jnp.zeros((16, 256), F32)
    field[0] = zero
    field[129] = zero
    pred[0] = zero
    flow_edges(field, fe)
    flow_halo = pair_copies(me, fe, fh, psem.at[0])
    solid_halo = pair_copies(me, se, sh, psem.at[1])
    start_all(flow_halo + solid_halo)

    scatter_wait(idr, isem, 1)
    answers(me, idr, solid, xs, xr, wl, xsem)

    loads[4].wait()
    loads[5].wait()
    wait_all(flow_halo)

    @pl.loop(0, 128 // ZB - 1)
    def _(n):
        predict_block(field, fh, vel, heat, pred, pe, pl.multiple_of(n * ZB, ZB), ZB)

    predict_block(field, fh, vel, heat, pred, pe, 128 - ZB, ZB - 1)
    pred_halo = pair_copies(me, pe, ph, psem.at[2])
    start_all(pred_halo)

    wait_all(solid_halo)
    solid_base(solid, cond, sh, s0, s1, cx)
    rest = pltpu.make_async_copy(
        s0.at[pl.ds(4, 28), pl.ds(0, 16)], solid_out.at[pl.ds(4, 28)], outsem.at[8]
    )
    rest.start()

    scatter_wait(xr, xsem, 1)
    forward(xr, fp, sd, rank, wk, lhs, acc, wall)

    field[129] = wall[...]
    pred[129] = wall[...]
    xlow = fh[0, 112:128, :].astype(F32)[15:16]
    xhigh = fh[1, 112:128, :].astype(F32)[15:16]
    centre, slope = slope_of(field, 128, xlow, xhigh, vel, heat, 127)
    top = centre + TIMESTEP * slope
    pred[128] = top
    pt[0] = top[0:1]
    pt[1] = top[15:16]
    top_halo = pair_copies(me, pt, pth, psem.at[3])
    start_all(top_halo)

    wait_all(pred_halo)

    def correct(n):
        z0 = pl.multiple_of(n * ZB, ZB)
        correct_block(pred, ph, vel, heat, field, z0, ZB)
        out = pl.ds(z0, ZB)
        pltpu.make_async_copy(field.at[pl.ds(z0 + 1, ZB)], flow_out.at[out], outsem.at[n]).start()

    @pl.loop(0, C_FIRST)
    def _(n):
        correct(n)

    wait_all(top_halo)
    centre, slope = slope_of(pred, 128, pth[0], pth[1], vel, heat, 127)
    done = 0.5 * field[128] + 0.5 * (centre + TIMESTEP * slope)
    field[128] = done
    flux = FILM_COEFF * (done - wall[...])
    backward(me, flux, wk, fp, sd, rank, wl, vs, zacc, z, zr, zsem)

    @pl.loop(C_FIRST, 128 // ZB - 1)
    def _(n):
        correct(n)

    correct_block(pred, ph, vel, heat, field, 128 - ZB, ZB - 1)
    last = 128 // ZB - 1
    pltpu.make_async_copy(
        field.at[pl.ds(129 - ZB, ZB)], flow_out.at[pl.ds(128 - ZB, ZB)], outsem.at[last]
    ).start()

    scatter_wait(zr, zsem, 1)
    total = gather_up(zr, idr, acc)
    ff[0] = total[0:4]
    ff[1] = total[12:16]
    face_halo = pair_copies(me, ff, ffh, psem.at[4])
    start_all(face_halo)
    wait_all(face_halo)
    response = flux_response(widen(total, ffh[1], ffh[0]), cx, t0, t1)
    solid[0:4] = s0[0:4, 0:16, :] + response[0:4, 0:16, :]
    near = pltpu.make_async_copy(solid.at[pl.ds(0, 4)], solid_out.at[pl.ds(0, 4)], outsem.at[9])
    near.start()

    @pl.loop(0, 128 // ZB)
    def _(n):
        out = pl.ds(pl.multiple_of(n * ZB, ZB), ZB)
        pltpu.make_async_copy(field.at[pl.ds(n * ZB + 1, ZB)], flow_out.at[out], outsem.at[n]).wait()

    scatter_wait(ids, isem, 0)
    scatter_wait(xs, xsem, 0)
    scatter_wait(z, zsem, 0)
    rest.wait()
    near.wait()


C_FIRST = 5
FU = 2
BU = 2
GU = 8
CODE = 32767.0 / 6.0


def hand_on_kernel(flow_in, solid_in, flow_out, solid_out, flow, solid, insem, outsem):
    first, second = [], []
    for n in range(8):
        part = pl.ds(n * 16, 16)
        first.append(pltpu.make_async_copy(flow_in.at[part], flow.at[part], insem.at[n]))
        second.append(pltpu.make_async_copy(flow.at[part], flow_out.at[part], outsem.at[n]))
    first.append(pltpu.make_async_copy(solid_in, solid, insem.at[8]))
    second.append(pltpu.make_async_copy(solid, solid_out, outsem.at[8]))
    start_all(first)
    for one, two in zip(first, second):
        one.wait()
        two.start()
    wait_all(second)


def hand_on(flow, solid):
    hbm = pl.BlockSpec(memory_space=pl.ANY)
    return pl.pallas_call(
        hand_on_kernel,
        out_shape=(
            jax.ShapeDtypeStruct((128, 16, 256), F32),
            jax.ShapeDtypeStruct((32, 16, 256), F32),
        ),
        in_specs=[hbm, hbm],
        out_specs=(hbm, hbm),
        scratch_shapes=[
            pltpu.VMEM((128, 16, 256), F32),
            pltpu.VMEM((32, 16, 256), F32),
            pltpu.SemaphoreType.DMA((9,)),
            pltpu.SemaphoreType.DMA((9,)),
        ],
        compiler_params=pltpu.CompilerParams(vmem_limit_bytes=60 * 1024 * 1024),
        name="hand_on",
    )(flow, solid)


def body(flow, vel, heat, solid, cond, table, fp, sd, sp, b):
    fp, sd, sp, b = (v.reshape(1, NK) for v in (fp, sd, sp, b))
    vm, hbm = pl.BlockSpec(memory_space=pltpu.VMEM), pl.BlockSpec(memory_space=pl.ANY)
    dma = pltpu.SemaphoreType.DMA
    scratch = [
        pltpu.VMEM((130, 16, 256), F32),
        pltpu.VMEM((130, 16, 256), F32),
        pltpu.VMEM((3, 128, 16, 256), BF16),
        pltpu.VMEM((128, 16, 256), BF16),
        pltpu.VMEM((32, 16, 256), F32),
        pltpu.VMEM((32, 16, 256), F32),
        pltpu.VMEM((256, 1024), F32),
        pltpu.VMEM((2, 256, 1024), BF16),
        pltpu.VMEM((256, NK), F32),
        pltpu.VMEM((16, 256), F32),
        pltpu.VMEM((16, 256), F32),
        pltpu.VMEM((1, NK), I32),
        pltpu.VMEM((DEV, 1, 128), F32),
        pltpu.VMEM((DEV, 1, 128), F32),
        pltpu.VMEM((DEV, 8, 128), I16),
        pltpu.VMEM((DEV, 8, 128), I16),
        pltpu.VMEM((DEV, 8, 128), F32),
        pltpu.VMEM((DEV, 8, 128), F32),
        pltpu.VMEM((512, 512), BF16),
        pltpu.VMEM((256, 32), BF16),
        pltpu.VMEM((2, 128, 256), BF16),
        pltpu.VMEM((2, 128, 256), BF16),
        pltpu.VMEM((2, 128, 256), BF16),
        pltpu.VMEM((2, 128, 256), BF16),
        pltpu.VMEM((2, 1, 256), F32),
        pltpu.VMEM((2, 1, 256), F32),
        pltpu.VMEM((2, 16, 16, 256), BF16),
        pltpu.VMEM((2, 16, 16, 256), BF16),
        pltpu.VMEM((2, 4, 256), F32),
        pltpu.VMEM((2, 4, 256), F32),
        pltpu.VMEM((32, 24, 256), F32),
        pltpu.VMEM((32, 24, 256), F32),
        pltpu.VMEM((32, 24, 256), F32),
        pltpu.VMEM((5, 24, 256), F32),
        pltpu.VMEM((5, 24, 256), F32),
        pltpu.VMEM((DEV, KT), F32),
        pltpu.VMEM((32, 256), F32),
        pltpu.VMEM((256, 16), F32),
        pltpu.VMEM((256, 256), F32),
        pltpu.VMEM((2, 16, NK), BF16),
        dma((6,)),
        dma((10,)),
        dma((2,)),
        dma((2,)),
        dma((2,)),
        dma((5, 4)),
    ]
    results = pl.pallas_call(
        kernel,
        out_shape=(
            jax.ShapeDtypeStruct((128, 16, 256), F32),
            jax.ShapeDtypeStruct((32, 16, 256), F32),
        ),
        in_specs=[hbm] * 6 + [vm] * 4,
        out_specs=(hbm, hbm),
        scratch_shapes=scratch,
        compiler_params=pltpu.CompilerParams(
            vmem_limit_bytes=60 * 1024 * 1024, collective_id=0, has_side_effects=True
        ),
        name="coupled",
    )(flow, vel, heat, solid, cond, table.reshape(256, 1024), fp, sd, sp, b)
    return hand_on(*results)


def solution(mesh):
    placed = (
        P(None, ("grp", "dom"), None),
        P(None, None, ("grp", "dom"), None),
        P(None, ("grp", "dom"), None),
        P(None, ("grp", "dom"), None),
        P(None, ("grp", "dom"), None),
        P(),
        P(("grp", "dom")),
        P(("grp", "dom"), None),
        P(("grp", "dom")),
        P(("grp", "dom")),
    )
    return jax.shard_map(
        body,
        mesh=mesh,
        in_specs=placed,
        out_specs=(P(None, ("grp", "dom"), None), P(None, ("grp", "dom"), None)),
        check_vma=False,
    )
```

```python
import jax
import jax.numpy as jnp
from jax import lax
from jax.experimental import pallas as pl
from jax.experimental.pallas import tpu as pltpu
from jax.sharding import PartitionSpec as P

MESH = pl.DeviceIdType.MESH
F32, BF16, I32, I16 = jnp.float32, jnp.bfloat16, jnp.int32, jnp.int16

SUBCYCLES = 4
DIFFUSION = 0.8
TIMESTEP = 0.12
FILM_COEFF = 1.0
CONDUCT_RATE = 0.08
FLUX_GAIN = 0.25

DEV = 128
KT = 256
NK = 4096
TILES = NK // KT
ZB = 16
NN = (((1,), (0,)), ((), ()))
NT = (((1,), (1,)), ((), ()))


def dot(a, b, dims=NN):
    return lax.dot_general(a, b, dims, preferred_element_type=F32)


def narrow(row):
    return jnp.broadcast_to(row, (16, row.shape[1])).astype(I16)


def onehot(row, rows):
    key = narrow(row)
    place = lax.broadcasted_iota(I32, key.shape, 0).astype(I16)
    one, zero = BF16(1), BF16(0)
    return jnp.concatenate(
        [jnp.where(place == key - I16(16 * v), one, zero) for v in range(rows // 16)], axis=0
    )


def spread(key, count, value):
    return spread_at(narrow(key), count, value)


def spread_at(key, count, value):
    return jnp.concatenate([jnp.where(key == I16(v), value, BF16(0)) for v in range(count)], axis=0)


def patch_keys(patch):
    return (patch >> 2) & 3, (patch & 3) * 16 + (patch >> 4)


def face_of(sums):
    turned = sums.T
    return jnp.concatenate(
        [
            turned[c % 4 * 16 : c % 4 * 16 + 16, c // 4 * 16 : c // 4 * 16 + 16]
            for c in range(16)
        ],
        axis=1,
    )


def choose(key, count, blocks):
    key = jnp.broadcast_to(key, (8, key.shape[1]))
    low = high = jnp.zeros(key.shape, F32)
    for v in range(count):
        mask = key == v
        low = jnp.where(mask, blocks[v * 16 : v * 16 + 8], low)
        high = jnp.where(mask, blocks[v * 16 + 8 : v * 16 + 16], high)
    return low, high


def split(value):
    high = value.astype(BF16)
    return high, (value - high.astype(F32)).astype(BF16)


def beside(value):
    high, low = split(value.T)
    return jnp.concatenate([high, low], axis=1)


def swap_halves(low, high):
    axis = low.ndim - 1
    left = lax.broadcasted_iota(I32, low.shape, axis) < 64
    return jnp.where(left, low, pltpu.roll(high, 64, axis)), jnp.where(
        left, pltpu.roll(low, 64, axis), high
    )


def encode(value):
    step = jnp.floor(jnp.clip(value * CODE, -32767.0, 32767.0) + 0.5)
    return step.astype(I32).astype(I16)


def tile_at(t, size=KT):
    return pl.ds(pl.multiple_of(t * size, size), size)


def coords(device):
    return (lax.div(device, 64), lax.rem(device, 64))


def peer(me, offset):
    return lax.rem(me + offset, DEV)


def remote(src, dst, send, recv, device):
    return pltpu.make_async_remote_copy(
        src_ref=src,
        dst_ref=dst,
        send_sem=send,
        recv_sem=recv,
        device_id=coords(device),
        device_id_type=MESH,
    )


def pair_copies(me, edges, halo, sems):
    up = remote(edges.at[1], halo.at[0], sems.at[0], sems.at[1], peer(me, 1))
    down = remote(edges.at[0], halo.at[1], sems.at[2], sems.at[3], peer(me, DEV - 1))
    return up, down


def start_all(copies):
    for copy in copies:
        copy.start()


def wait_all(copies):
    for copy in copies:
        copy.wait()


def scatter_one(me, to, src, dst, sems):
    remote(src.at[to], dst.at[me], sems.at[0], sems.at[1], to).start()


def scatter_start(me, src, dst, sems):
    for o in range(1, 8):
        scatter_one(me, peer(me, o), src, dst, sems)

    @pl.loop(1, DEV // 8)
    def _(n):
        for q in range(8):
            scatter_one(me, peer(me, n * 8 + q), src, dst, sems)

    dst[me] = src[me]


def scatter_wait(ref, sems, which):
    many = ref.at[pl.ds(0, DEV - 1)]
    pltpu.make_async_copy(many, many, sems.at[which]).wait()


def rank_and_ids(sd_ref, sp_ref, rank, ids, carry, acc, beside_it):
    before = lax.broadcasted_iota(I32, (KT, KT), 0) < lax.broadcasted_iota(I32, (KT, KT), 1)
    before = jnp.where(before, 1.0, 0.0).astype(BF16)
    every = jnp.ones((KT, KT), BF16)
    carry[...] = jnp.zeros_like(carry)
    acc[...] = jnp.zeros_like(acc)

    @pl.loop(0, TILES // 4)
    def _(n):
        beside_it(n)
        held, total = carry[...], jnp.zeros((32, 256), F32)
        for u in range(4):
            k = tile_at(n * 4 + u)
            sd = sd_ref[:, k]
            mine = lax.broadcasted_iota(I32, (DEV, KT), 0) == sd
            one = onehot(sd, DEV)
            ahead = dot(one, before) + held
            r = jnp.sum(jnp.where(mine, ahead, 0.0), axis=0, keepdims=True).astype(I32)
            held = held + dot(one, every)
            rank[:, k] = r
            tag = (sp_ref[:, k] + 1).astype(F32)
            place = lax.broadcasted_iota(I32, (32, KT), 0)
            m = jnp.where(place == (sd & 31), tag, 0.0).astype(BF16)
            total = total + dot(m, onehot((sd >> 5) * 64 + r, 256), NT)
        carry[...] = held
        acc[...] += total

    got = acc[...]
    left = lax.broadcasted_iota(I32, (32, 128), 1) < 64
    for t in range(2):
        both = got[:, t * 128 : (t + 1) * 128]
        turned = pltpu.roll(both, 64, 1)
        ids[t * 64 : t * 64 + 32] = jnp.where(left, both, turned).reshape(32, 1, 128)
        ids[t * 64 + 32 : t * 64 + 64] = jnp.where(left, turned, both).reshape(32, 1, 128)


def flow_edges(field, edges):
    @pl.loop(0, 128 // ZB)
    def _(b):
        z0 = pl.multiple_of(b * ZB, ZB)
        block = field[pl.ds(z0 + 1, ZB)]
        edges[0, pl.ds(z0, ZB), :] = block[:, 0, :].astype(BF16)
        edges[1, pl.ds(z0, ZB), :] = block[:, 15, :].astype(BF16)


def solid_edges(solid, cond, edges):
    low = jnp.concatenate([solid[:, 0:4, :], cond[:, 0:4, :]], axis=1)
    high = jnp.concatenate([solid[:, 12:16, :], cond[:, 12:16, :]], axis=1)
    edges[0] = low.reshape(16, 16, 256).astype(BF16)
    edges[1] = high.reshape(16, 16, 256).astype(BF16)


def pick_tags(idr, s):
    left = lax.broadcasted_iota(I32, (1, 128), 1) < 64
    pairs = [jnp.where(left, idr[s + 2 * p], idr[s + 2 * p + 1]) for p in range(2)]
    return jnp.concatenate(pairs, axis=1).astype(I32) - 1


def answers(me, idr, solid, xs, xr, wl, sems):
    wl[...] = beside(solid[0])
    first, turn = lax.div(me, 16), lax.rem(me, 16)

    def send(n):
        base = lax.rem(first + n, 8) * 16

        @pl.loop(0, 16)
        def _(q):
            to = base + lax.rem(turn + q, 16)

            @pl.when(to != me)
            def _():
                scatter_one(me, to, xs, xr, sems)

    @pl.loop(0, 8)
    def _(n):
        @pl.when(n > 0)
        def _():
            send(n + 7)

        base = lax.rem(first + n, 8) * 16
        for u in range(4):
            s = base + u * 4
            tag = pick_tags(idr, s)
            row = onehot(tag >> 4, 16)
            blocks = dot(wl[...], jnp.concatenate([row, row], axis=0))
            low, high = choose(tag & 15, 16, blocks)
            for p in range(2):
                lanes = slice(p * 128, (p + 1) * 128)
                one, two = swap_halves(low[:, lanes], high[:, lanes])
                xs[s + 2 * p] = encode(one)
                xs[s + 2 * p + 1] = encode(two)

    send(7)
    xr[me] = xs[me]


def weights(tab, b_ref, wk):
    @pl.loop(0, TILES)
    def _(t):
        k = tile_at(t)
        block = onehot(b_ref[:, k], 1024)
        wk[:, k] = dot(tab[0], block) + dot(tab[1], block)


def forward(xr, fp_ref, sd_ref, rank, wk, lhs, acc, face):
    for t in range(2):
        d = t * 64
        one = xr[d : d + 32].astype(I32).astype(F32)
        two = xr[d + 32 : d + 64].astype(I32).astype(F32)
        both = jnp.concatenate(swap_halves(one, two), axis=1).reshape(512, 128)
        high, low = split(both)
        lhs[:, t * 128 : (t + 1) * 128] = high
        lhs[:, 256 + t * 128 : 256 + (t + 1) * 128] = low
    acc[...] = jnp.zeros_like(acc)

    @pl.loop(0, TILES // FU)
    def _(n):
        spreads, rows = [], []
        for u in range(FU):
            k = tile_at(n * FU + u)
            fp, sd, r = fp_ref[:, k], sd_ref[:, k], rank[:, k]
            slot = onehot((sd >> 5) * 64 + r, 256)
            blocks = dot(lhs[...], jnp.concatenate([slot, slot], axis=0))
            low, high = choose(sd & 31, 32, blocks)
            w = wk[:, k]
            y = jnp.concatenate(
                [
                    jnp.sum(
                        w[i * 16 : i * 16 + 8] * low + w[i * 16 + 8 : i * 16 + 16] * high,
                        axis=0,
                        keepdims=True,
                    )
                    for i in range(16)
                ],
                axis=0,
            )
            block, column = patch_keys(fp)
            block, row = narrow(block), onehot(column, 64)
            for part in split(y * (1.0 / CODE)):
                spreads.append(spread_at(block, 4, part))
                rows.append(row)
        acc[...] += dot(jnp.concatenate(spreads, axis=1), jnp.concatenate(rows, axis=1), NT)

    face[...] = face_of(acc[...])


def backward(me, flux, wk, fp_ref, sd_ref, rank, fl, vs, acc, z, zr, sems):
    fl[...] = beside(flux)

    @pl.loop(0, TILES // BU)
    def _(n):
        for u in range(BU):
            k = tile_at(n * BU + u)
            fp = fp_ref[:, k]
            row = onehot(fp >> 4, 16)
            low, high = choose(fp & 15, 16, dot(fl[...], jnp.concatenate([row, row], axis=0)))
            value = jnp.zeros((16, KT), F32)
            for i in range(16):
                y = low[i : i + 1] if i < 8 else high[i - 8 : i - 7]
                value = value + wk[i * 16 : (i + 1) * 16, k] * y
            vs[0, :, k], vs[1, :, k] = split(value)

    turn = lax.rem(me, 64)

    def send(half, i):
        j = lax.rem(turn + i, 64)
        to = lax.div(j, 16) * 32 + half * 16 + lax.rem(j, 16)

        @pl.when(to != me)
        def _():
            scatter_one(me, to, z, zr, sems)

    for half in range(2):
        acc[...] = jnp.zeros_like(acc)

        @pl.loop(0, TILES // 4)
        def _(n):
            if half:
                for i in range(16):
                    send(0, n * 16 + i)
            spreads, slots = [], []
            for u in range(4):
                k = tile_at(n * 4 + u)
                sd, r = sd_ref[:, k], rank[:, k]
                slots.append(onehot((sd >> 5) * 64 + r, 256))
                e = narrow((sd & 31) - half * 16)
                spreads.append(
                    jnp.concatenate([spread_at(e, 16, vs[part, :, k]) for part in range(2)], axis=0)
                )
            acc[...] += dot(jnp.concatenate(spreads, axis=1), jnp.concatenate(slots, axis=1), NT)

        got = acc[0:256] + acc[256:512]
        for t in range(2):
            both = got[:, t * 128 : (t + 1) * 128].reshape(16, 16, 128)
            d = t * 64 + half * 16
            z[d : d + 16], z[d + 32 : d + 48] = swap_halves(both[:, 0:8], both[:, 8:16])

    @pl.loop(0, 16)
    def _(n):
        for i in range(4):
            send(1, n * 4 + i)

    zr[me] = z[me]


def gather_keys(idr, blocks, columns):
    @pl.loop(0, DEV // 16)
    def _(n):
        for u in range(4):
            t = n * 4 + u
            block, column = patch_keys(pick_tags(idr, t * 4))
            blocks[:, tile_at(t)] = narrow(block)
            columns[:, tile_at(t)] = onehot(column, 64)


def gather_up(zr, blocks, columns, acc):
    acc[...] = jnp.zeros_like(acc)

    @pl.loop(0, DEV // 4 // GU)
    def _(n):
        spreads, rows = [], []
        for u in range(GU):
            t = n * GU + u
            s = t * 4
            lows, highs = [], []
            for p in range(2):
                low, high = swap_halves(zr[s + 2 * p], zr[s + 2 * p + 1])
                lows.append(low)
                highs.append(high)
            value = jnp.concatenate(
                [jnp.concatenate(lows, axis=1), jnp.concatenate(highs, axis=1)], axis=0
            )
            block, row = blocks[:, tile_at(t)], columns[:, tile_at(t)]
            for part in split(value):
                spreads.append(spread_at(block, 4, part))
                rows.append(row)
        acc[...] += dot(jnp.concatenate(spreads, axis=1), jnp.concatenate(rows, axis=1), NT)

    return face_of(acc[...]) * FLUX_GAIN


def slope_of(field, index, xlow, xhigh, vel, heat, z):
    centre = field[index]
    rows = lax.broadcasted_iota(I32, (16, 256), 0)
    xbelow = jnp.where(rows == 0, xlow, pltpu.roll(centre, 1, 0))
    xabove = jnp.where(rows == 15, xhigh, pltpu.roll(centre, 15, 0))
    sides = (
        (field[index - 1], field[index + 1]),
        (xbelow, xabove),
        (pltpu.roll(centre, 1, 1), pltpu.roll(centre, 255, 1)),
    )
    total = heat[z].astype(F32)
    for axis, (below, above) in enumerate(sides):
        c = vel[axis, z].astype(F32)
        weight = jnp.maximum(c, 0.0) + DIFFUSION
        total = total + (below - centre) * weight + (above - centre) * (weight - c)
    return centre, total


def predict_block(field, halo, vel, heat, pred, edges, z0, count):
    xlow = halo[0, pl.ds(z0, ZB), :].astype(F32)
    xhigh = halo[1, pl.ds(z0, ZB), :].astype(F32)
    first, last = [], []
    for q in range(count):
        z = z0 + q
        centre, slope = slope_of(
            field, z + 1, xlow[q : q + 1], xhigh[q : q + 1], vel, heat, z
        )
        value = centre + TIMESTEP * slope
        pred[z + 1] = value
        first.append(value[0:1])
        last.append(value[15:16])
    for _ in range(count, ZB):
        first.append(jnp.zeros((1, 256), F32))
        last.append(jnp.zeros((1, 256), F32))
    edges[0, pl.ds(z0, ZB), :] = jnp.concatenate(first, axis=0).astype(BF16)
    edges[1, pl.ds(z0, ZB), :] = jnp.concatenate(last, axis=0).astype(BF16)


def correct_block(pred, halo, vel, heat, field, z0, count):
    xlow = halo[0, pl.ds(z0, ZB), :].astype(F32)
    xhigh = halo[1, pl.ds(z0, ZB), :].astype(F32)
    for q in range(count):
        z = z0 + q
        centre, slope = slope_of(pred, z + 1, xlow[q : q + 1], xhigh[q : q + 1], vel, heat, z)
        field[z + 1] = 0.5 * field[z + 1] + 0.5 * (centre + TIMESTEP * slope)


def widen(own, above, below):
    return jnp.concatenate([own, above, below], axis=own.ndim - 2)


def spread_of(src, z, layers):
    centre = src[z]
    zbelow = src[max(z - 1, 0)]
    zabove = src[z + 1] if z + 1 < layers else jnp.zeros_like(centre)
    total = zbelow + zabove + pltpu.roll(centre, 1, 0) + pltpu.roll(centre, 23, 0)
    return centre, total + pltpu.roll(centre, 1, 1) + pltpu.roll(centre, 255, 1) - 6.0 * centre


def solid_base(solid, cond, halo, s0, s1, cx):
    below = halo[0].astype(F32).reshape(32, 8, 256)
    above = halo[1].astype(F32).reshape(32, 8, 256)
    s0[...] = widen(solid[...], above[:, 0:4], below[:, 0:4])
    cx[...] = CONDUCT_RATE * widen(cond[...], above[:, 4:8], below[:, 4:8])
    src, dst = s0, s1
    for step in range(SUBCYCLES):
        for z in range(32):
            centre, total = spread_of(src, z, 32)
            dst[z] = centre + cx[z] * total
        src, dst = dst, src


def flux_response(wide, cx, t0, t1):
    t0[...] = jnp.zeros_like(t0)
    t1[...] = jnp.zeros_like(t1)
    t0[0] = wide
    src, dst = t0, t1
    for step in range(1, SUBCYCLES):
        for z in range(step + 1):
            centre, total = spread_of(src, z, 5)
            value = centre + cx[z] * total
            dst[z] = value + wide if z == 0 else value
        src, dst = dst, src
    return src


def kernel(
    flow_in, vel_in, heat_in, solid_in, cond_in, table_in, fp, sd, sp, b,
    flow_out, solid_out,
    field, pred, vel, heat, solid, cond, table, tab, wk, wall, wallt,
    rank, ids, idr, xs, xr, z, zr, lhs, wl,
    fe, fh, pe, ph, pt, pth, se, sh, ff, ffh,
    s0, s1, cx, t0, t1, carry, idacc, acc, zacc, vs, blocks, columns,
    insem, outsem, isem, xsem, zsem, psem,
):
    me = lax.axis_index("grp") * 64 + lax.axis_index("dom")
    barrier = pltpu.get_barrier_semaphore()

    loads = [
        pltpu.make_async_copy(src, dst, insem.at[i])
        for i, (src, dst) in enumerate(
            (
                (solid_in, solid),
                (cond_in, cond),
                (flow_in, field.at[pl.ds(1, 128)]),
                (table_in, table),
                (vel_in, vel),
                (heat_in, heat),
            )
        )
    ]
    start_all(loads)

    def greet(n):
        for q in range(32):
            to = peer(me, n * 32 + q)
            if q:
                pl.semaphore_signal(barrier, inc=1, device_id=coords(to), device_id_type=MESH)
            else:

                @pl.when(n > 0)
                def _():
                    pl.semaphore_signal(barrier, inc=1, device_id=coords(to), device_id_type=MESH)

    rank_and_ids(sd, sp, rank, ids, carry, idacc, greet)
    loads[3].wait()
    tab[0], tab[1] = split(table[...])
    loads[0].wait()
    loads[1].wait()
    solid_edges(solid, cond, se)
    loads[2].wait()
    zero = jnp.zeros((16, 256), F32)
    field[0] = zero
    field[129] = zero
    pred[0] = zero
    flow_edges(field, fe)
    pl.semaphore_wait(barrier, DEV - 1)

    scatter_start(me, ids, idr, isem)
    flow_halo = pair_copies(me, fe, fh, psem.at[0])
    solid_halo = pair_copies(me, se, sh, psem.at[1])
    start_all(flow_halo + solid_halo)
    weights(tab, b, wk)

    scatter_wait(idr, isem, 1)
    answers(me, idr, solid, xs, xr, wl, xsem)

    loads[4].wait()
    loads[5].wait()
    wait_all(flow_halo)

    @pl.loop(0, 128 // ZB - 1)
    def _(n):
        predict_block(field, fh, vel, heat, pred, pe, pl.multiple_of(n * ZB, ZB), ZB)

    predict_block(field, fh, vel, heat, pred, pe, 128 - ZB, ZB - 1)
    pred_halo = pair_copies(me, pe, ph, psem.at[2])
    start_all(pred_halo)

    wait_all(solid_halo)
    solid_base(solid, cond, sh, s0, s1, cx)
    rest = pltpu.make_async_copy(
        s0.at[pl.ds(4, 28), pl.ds(0, 16)], solid_out.at[pl.ds(4, 28)], outsem.at[8]
    )
    rest.start()

    scatter_wait(xr, xsem, 1)
    forward(xr, fp, sd, rank, wk, lhs, acc, wall)

    field[129] = wall[...]
    pred[129] = wall[...]
    xlow = fh[0, 112:128, :].astype(F32)[15:16]
    xhigh = fh[1, 112:128, :].astype(F32)[15:16]
    centre, slope = slope_of(field, 128, xlow, xhigh, vel, heat, 127)
    top = centre + TIMESTEP * slope
    pred[128] = top
    pt[0] = top[0:1]
    pt[1] = top[15:16]
    top_halo = pair_copies(me, pt, pth, psem.at[3])
    start_all(top_halo)

    wait_all(pred_halo)

    def correct(n):
        z0 = pl.multiple_of(n * ZB, ZB)
        correct_block(pred, ph, vel, heat, field, z0, ZB)
        out = pl.ds(z0, ZB)
        pltpu.make_async_copy(field.at[pl.ds(z0 + 1, ZB)], flow_out.at[out], outsem.at[n]).start()

    @pl.loop(0, C_FIRST)
    def _(n):
        correct(n)

    wait_all(top_halo)
    centre, slope = slope_of(pred, 128, pth[0], pth[1], vel, heat, 127)
    done = 0.5 * field[128] + 0.5 * (centre + TIMESTEP * slope)
    field[128] = done
    flux = FILM_COEFF * (done - wall[...])
    backward(me, flux, wk, fp, sd, rank, wl, vs, zacc, z, zr, zsem)

    @pl.loop(C_FIRST, 128 // ZB - 1)
    def _(n):
        correct(n)

    correct_block(pred, ph, vel, heat, field, 128 - ZB, ZB - 1)
    last = 128 // ZB - 1
    pltpu.make_async_copy(
        field.at[pl.ds(129 - ZB, ZB)], flow_out.at[pl.ds(128 - ZB, ZB)], outsem.at[last]
    ).start()

    gather_keys(idr, blocks, columns)
    scatter_wait(zr, zsem, 1)
    total = gather_up(zr, blocks, columns, acc)
    ff[0] = total[0:4]
    ff[1] = total[12:16]
    face_halo = pair_copies(me, ff, ffh, psem.at[4])
    start_all(face_halo)
    wait_all(face_halo)
    response = flux_response(widen(total, ffh[1], ffh[0]), cx, t0, t1)
    solid[0:4] = s0[0:4, 0:16, :] + response[0:4, 0:16, :]
    near = pltpu.make_async_copy(solid.at[pl.ds(0, 4)], solid_out.at[pl.ds(0, 4)], outsem.at[9])
    near.start()

    @pl.loop(0, 128 // ZB)
    def _(n):
        out = pl.ds(pl.multiple_of(n * ZB, ZB), ZB)
        pltpu.make_async_copy(field.at[pl.ds(n * ZB + 1, ZB)], flow_out.at[out], outsem.at[n]).wait()

    scatter_wait(ids, isem, 0)
    scatter_wait(xs, xsem, 0)
    scatter_wait(z, zsem, 0)
    rest.wait()
    near.wait()


C_FIRST = 5
FU = 4
BU = 4
GU = 8
CODE = 32767.0 / 6.0


def hand_on_kernel(flow_in, solid_in, flow_out, solid_out, flow, solid, insem, outsem):
    first, second = [], []
    for n in range(8):
        part = pl.ds(n * 16, 16)
        first.append(pltpu.make_async_copy(flow_in.at[part], flow.at[part], insem.at[n]))
        second.append(pltpu.make_async_copy(flow.at[part], flow_out.at[part], outsem.at[n]))
    first.append(pltpu.make_async_copy(solid_in, solid, insem.at[8]))
    second.append(pltpu.make_async_copy(solid, solid_out, outsem.at[8]))
    start_all(first)
    for one, two in zip(first, second):
        one.wait()
        two.start()
    wait_all(second)


def hand_on(flow, solid):
    hbm = pl.BlockSpec(memory_space=pl.ANY)
    return pl.pallas_call(
        hand_on_kernel,
        out_shape=(
            jax.ShapeDtypeStruct((128, 16, 256), F32),
            jax.ShapeDtypeStruct((32, 16, 256), F32),
        ),
        in_specs=[hbm, hbm],
        out_specs=(hbm, hbm),
        scratch_shapes=[
            pltpu.VMEM((128, 16, 256), F32),
            pltpu.VMEM((32, 16, 256), F32),
            pltpu.SemaphoreType.DMA((9,)),
            pltpu.SemaphoreType.DMA((9,)),
        ],
        compiler_params=pltpu.CompilerParams(vmem_limit_bytes=60 * 1024 * 1024),
        name="hand_on",
    )(flow, solid)


def body(flow, vel, heat, solid, cond, table, fp, sd, sp, b):
    fp, sd, sp, b = (v.reshape(1, NK) for v in (fp, sd, sp, b))
    vm, hbm = pl.BlockSpec(memory_space=pltpu.VMEM), pl.BlockSpec(memory_space=pl.ANY)
    dma = pltpu.SemaphoreType.DMA
    scratch = [
        pltpu.VMEM((130, 16, 256), F32),
        pltpu.VMEM((130, 16, 256), F32),
        pltpu.VMEM((3, 128, 16, 256), BF16),
        pltpu.VMEM((128, 16, 256), BF16),
        pltpu.VMEM((32, 16, 256), F32),
        pltpu.VMEM((32, 16, 256), F32),
        pltpu.VMEM((256, 1024), F32),
        pltpu.VMEM((2, 256, 1024), BF16),
        pltpu.VMEM((256, NK), F32),
        pltpu.VMEM((16, 256), F32),
        pltpu.VMEM((16, 256), F32),
        pltpu.VMEM((1, NK), I32),
        pltpu.VMEM((DEV, 1, 128), F32),
        pltpu.VMEM((DEV, 1, 128), F32),
        pltpu.VMEM((DEV, 8, 128), I16),
        pltpu.VMEM((DEV, 8, 128), I16),
        pltpu.VMEM((DEV, 8, 128), F32),
        pltpu.VMEM((DEV, 8, 128), F32),
        pltpu.VMEM((512, 512), BF16),
        pltpu.VMEM((256, 32), BF16),
        pltpu.VMEM((2, 128, 256), BF16),
        pltpu.VMEM((2, 128, 256), BF16),
        pltpu.VMEM((2, 128, 256), BF16),
        pltpu.VMEM((2, 128, 256), BF16),
        pltpu.VMEM((2, 1, 256), F32),
        pltpu.VMEM((2, 1, 256), F32),
        pltpu.VMEM((2, 16, 16, 256), BF16),
        pltpu.VMEM((2, 16, 16, 256), BF16),
        pltpu.VMEM((2, 4, 256), F32),
        pltpu.VMEM((2, 4, 256), F32),
        pltpu.VMEM((32, 24, 256), F32),
        pltpu.VMEM((32, 24, 256), F32),
        pltpu.VMEM((32, 24, 256), F32),
        pltpu.VMEM((5, 24, 256), F32),
        pltpu.VMEM((5, 24, 256), F32),
        pltpu.VMEM((DEV, KT), F32),
        pltpu.VMEM((32, 256), F32),
        pltpu.VMEM((64, 64), F32),
        pltpu.VMEM((512, 256), F32),
        pltpu.VMEM((2, 16, NK), BF16),
        pltpu.VMEM((16, 2 * NK), I16),
        pltpu.VMEM((64, 2 * NK), BF16),
        dma((6,)),
        dma((10,)),
        dma((2,)),
        dma((2,)),
        dma((2,)),
        dma((5, 4)),
    ]
    results = pl.pallas_call(
        kernel,
        out_shape=(
            jax.ShapeDtypeStruct((128, 16, 256), F32),
            jax.ShapeDtypeStruct((32, 16, 256), F32),
        ),
        in_specs=[hbm] * 6 + [vm] * 4,
        out_specs=(hbm, hbm),
        scratch_shapes=scratch,
        compiler_params=pltpu.CompilerParams(
            vmem_limit_bytes=60 * 1024 * 1024, collective_id=0, has_side_effects=True
        ),
        name="coupled",
    )(flow, vel, heat, solid, cond, table.reshape(256, 1024), fp, sd, sp, b)
    return hand_on(*results)


def solution(mesh):
    placed = (
        P(None, ("grp", "dom"), None),
        P(None, None, ("grp", "dom"), None),
        P(None, ("grp", "dom"), None),
        P(None, ("grp", "dom"), None),
        P(None, ("grp", "dom"), None),
        P(),
        P(("grp", "dom")),
        P(("grp", "dom"), None),
        P(("grp", "dom")),
        P(("grp", "dom")),
    )
    return jax.shard_map(
        body,
        mesh=mesh,
        in_specs=placed,
        out_specs=(P(None, ("grp", "dom"), None), P(None, ("grp", "dom"), None)),
        check_vma=False,
    )
```

```python
import jax
import jax.numpy as jnp
from jax import lax
from jax.experimental import pallas as pl
from jax.experimental.pallas import tpu as pltpu
from jax.sharding import PartitionSpec as P

MESH = pl.DeviceIdType.MESH
F32, BF16, I32, I16 = jnp.float32, jnp.bfloat16, jnp.int32, jnp.int16

SUBCYCLES = 4
DIFFUSION = 0.8
TIMESTEP = 0.12
FILM_COEFF = 1.0
CONDUCT_RATE = 0.08
FLUX_GAIN = 0.25

DEV = 128
KT = 256
NK = 4096
TILES = NK // KT
ZB = 16
NN = (((1,), (0,)), ((), ()))
NT = (((1,), (1,)), ((), ()))


def dot(a, b, dims=NN):
    return lax.dot_general(a, b, dims, preferred_element_type=F32)


def narrow(row):
    return jnp.broadcast_to(row, (16, row.shape[1])).astype(I16)


def onehot(row, rows):
    key = narrow(row)
    place = lax.broadcasted_iota(I32, key.shape, 0).astype(I16)
    one, zero = BF16(1), BF16(0)
    return jnp.concatenate(
        [jnp.where(place == key - I16(16 * v), one, zero) for v in range(rows // 16)], axis=0
    )


def spread(key, count, value):
    return spread_at(narrow(key), count, value)


def spread_at(key, count, value):
    return jnp.concatenate([jnp.where(key == I16(v), value, BF16(0)) for v in range(count)], axis=0)


def patch_keys(patch):
    return (patch >> 2) & 3, (patch & 3) * 16 + (patch >> 4)


def face_of(sums):
    turned = sums.T
    return jnp.concatenate(
        [
            turned[c % 4 * 16 : c % 4 * 16 + 16, c // 4 * 16 : c // 4 * 16 + 16]
            for c in range(16)
        ],
        axis=1,
    )


def choose(key, count, blocks):
    key = jnp.broadcast_to(key, (8, key.shape[1]))
    low = high = jnp.zeros(key.shape, F32)
    for v in range(count):
        mask = key == v
        low = jnp.where(mask, blocks[v * 16 : v * 16 + 8], low)
        high = jnp.where(mask, blocks[v * 16 + 8 : v * 16 + 16], high)
    return low, high


def split(value):
    high = value.astype(BF16)
    return high, (value - high.astype(F32)).astype(BF16)


def beside(value):
    high, low = split(value.T)
    return jnp.concatenate([high, low], axis=1)


def swap_halves(low, high):
    axis = low.ndim - 1
    left = lax.broadcasted_iota(I32, low.shape, axis) < 64
    return jnp.where(left, low, pltpu.roll(high, 64, axis)), jnp.where(
        left, pltpu.roll(low, 64, axis), high
    )


def encode(value):
    step = jnp.floor(jnp.clip(value * CODE, -32767.0, 32767.0) + 0.5)
    return step.astype(I32).astype(I16)


def tile_at(t, size=KT):
    return pl.ds(pl.multiple_of(t * size, size), size)


def coords(device):
    return (lax.div(device, 64), lax.rem(device, 64))


def peer(me, offset):
    return lax.rem(me + offset, DEV)


def remote(src, dst, send, recv, device):
    return pltpu.make_async_remote_copy(
        src_ref=src,
        dst_ref=dst,
        send_sem=send,
        recv_sem=recv,
        device_id=coords(device),
        device_id_type=MESH,
    )


def pair_copies(me, edges, halo, sems):
    up = remote(edges.at[1], halo.at[0], sems.at[0], sems.at[1], peer(me, 1))
    down = remote(edges.at[0], halo.at[1], sems.at[2], sems.at[3], peer(me, DEV - 1))
    return up, down


def start_all(copies):
    for copy in copies:
        copy.start()


def wait_all(copies):
    for copy in copies:
        copy.wait()


def scatter_one(me, to, src, dst, sems):
    remote(src.at[to], dst.at[me], sems.at[0], sems.at[1], to).start()


def scatter_start(me, src, dst, sems):
    for o in range(1, 8):
        scatter_one(me, peer(me, o), src, dst, sems)

    @pl.loop(1, DEV // 8)
    def _(n):
        for q in range(8):
            scatter_one(me, peer(me, n * 8 + q), src, dst, sems)

    dst[me] = src[me]


def scatter_wait(ref, sems, which):
    many = ref.at[pl.ds(0, DEV - 1)]
    pltpu.make_async_copy(many, many, sems.at[which]).wait()


def rank_and_ids(sd_ref, sp_ref, rank, ids, carry, acc, beside_it):
    before = lax.broadcasted_iota(I32, (KT, KT), 0) < lax.broadcasted_iota(I32, (KT, KT), 1)
    before = jnp.where(before, 1.0, 0.0).astype(BF16)
    every = jnp.ones((KT, KT), BF16)
    carry[...] = jnp.zeros_like(carry)
    acc[...] = jnp.zeros_like(acc)

    @pl.loop(0, TILES // 4)
    def _(n):
        beside_it(n)
        held, total = carry[...], jnp.zeros((32, 256), F32)
        for u in range(4):
            k = tile_at(n * 4 + u)
            sd = sd_ref[:, k]
            mine = lax.broadcasted_iota(I32, (DEV, KT), 0) == sd
            one = onehot(sd, DEV)
            ahead = dot(one, before) + held
            r = jnp.sum(jnp.where(mine, ahead, 0.0), axis=0, keepdims=True).astype(I32)
            held = held + dot(one, every)
            rank[:, k] = r
            tag = (sp_ref[:, k] + 1).astype(F32)
            place = lax.broadcasted_iota(I32, (32, KT), 0)
            m = jnp.where(place == (sd & 31), tag, 0.0).astype(BF16)
            total = total + dot(m, onehot((sd >> 5) * 64 + r, 256), NT)
        carry[...] = held
        acc[...] += total

    got = acc[...]
    left = lax.broadcasted_iota(I32, (32, 128), 1) < 64
    for t in range(2):
        both = got[:, t * 128 : (t + 1) * 128]
        turned = pltpu.roll(both, 64, 1)
        ids[t * 64 : t * 64 + 32] = jnp.where(left, both, turned).reshape(32, 1, 128)
        ids[t * 64 + 32 : t * 64 + 64] = jnp.where(left, turned, both).reshape(32, 1, 128)


def flow_edges(field, edges):
    @pl.loop(0, 128 // ZB)
    def _(b):
        z0 = pl.multiple_of(b * ZB, ZB)
        block = field[pl.ds(z0 + 1, ZB)]
        edges[0, pl.ds(z0, ZB), :] = block[:, 0, :].astype(BF16)
        edges[1, pl.ds(z0, ZB), :] = block[:, 15, :].astype(BF16)


def solid_edges(solid, cond, edges):
    low = jnp.concatenate([solid[:, 0:4, :], cond[:, 0:4, :]], axis=1)
    high = jnp.concatenate([solid[:, 12:16, :], cond[:, 12:16, :]], axis=1)
    edges[0] = low.reshape(16, 16, 256).astype(BF16)
    edges[1] = high.reshape(16, 16, 256).astype(BF16)


def pick_tags(idr, s):
    left = lax.broadcasted_iota(I32, (1, 128), 1) < 64
    pairs = [jnp.where(left, idr[s + 2 * p], idr[s + 2 * p + 1]) for p in range(2)]
    return jnp.concatenate(pairs, axis=1).astype(I32) - 1


def answers(me, idr, solid, xs, xr, wl, sems):
    wl[...] = beside(solid[0])
    first, turn = lax.div(me, 16), lax.rem(me, 16)

    def send(n, q):
        to = lax.rem(first + n, 8) * 16 + lax.rem(turn + q, 16)
        scatter_one(me, to, xs, xr, sems)

    def group(n):
        base = lax.rem(first + n, 8) * 16
        for u in range(4):
            s = base + u * 4
            tag = pick_tags(idr, s)
            row = onehot(tag >> 4, 16)
            blocks = dot(wl[...], jnp.concatenate([row, row], axis=0))
            low, high = choose(tag & 15, 16, blocks)
            for p in range(2):
                lanes = slice(p * 128, (p + 1) * 128)
                one, two = swap_halves(low[:, lanes], high[:, lanes])
                xs[s + 2 * p] = encode(one)
                xs[s + 2 * p + 1] = encode(two)

    group(0)
    for q in range(1, 16):
        send(0, q)
    group(1)

    @pl.loop(1, 7)
    def _(n):
        for q in range(16):
            send(n, q)
        group(n + 1)

    for q in range(16):
        send(7, q)
    xr[me] = xs[me]


def weights(tab, b_ref, wk):
    @pl.loop(0, TILES)
    def _(t):
        k = tile_at(t)
        block = onehot(b_ref[:, k], 1024)
        wk[:, k] = dot(tab[0], block) + dot(tab[1], block)


def forward(xr, fp_ref, sd_ref, rank, wk, lhs, acc, face):
    for t in range(2):
        d = t * 64
        one = xr[d : d + 32].astype(I32).astype(F32)
        two = xr[d + 32 : d + 64].astype(I32).astype(F32)
        both = jnp.concatenate(swap_halves(one, two), axis=1).reshape(512, 128)
        high, low = split(both)
        lhs[:, t * 128 : (t + 1) * 128] = high
        lhs[:, 256 + t * 128 : 256 + (t + 1) * 128] = low
    acc[...] = jnp.zeros_like(acc)

    @pl.loop(0, TILES // FU)
    def _(n):
        spreads, rows = [], []
        for u in range(FU):
            k = tile_at(n * FU + u)
            fp, sd, r = fp_ref[:, k], sd_ref[:, k], rank[:, k]
            slot = onehot((sd >> 5) * 64 + r, 256)
            blocks = dot(lhs[...], jnp.concatenate([slot, slot], axis=0))
            low, high = choose(sd & 31, 32, blocks)
            w = wk[:, k]
            y = jnp.concatenate(
                [
                    jnp.sum(
                        w[i * 16 : i * 16 + 8] * low + w[i * 16 + 8 : i * 16 + 16] * high,
                        axis=0,
                        keepdims=True,
                    )
                    for i in range(16)
                ],
                axis=0,
            )
            block, column = patch_keys(fp)
            block, row = narrow(block), onehot(column, 64)
            for part in split(y * (1.0 / CODE)):
                spreads.append(spread_at(block, 4, part))
                rows.append(row)
        acc[...] += dot(jnp.concatenate(spreads, axis=1), jnp.concatenate(rows, axis=1), NT)

    face[...] = face_of(acc[...])


def backward(me, flux, wk, fp_ref, sd_ref, rank, fl, vs, acc, z, zr, sems):
    fl[...] = beside(flux)

    @pl.loop(0, TILES // BU)
    def _(n):
        for u in range(BU):
            k = tile_at(n * BU + u)
            fp = fp_ref[:, k]
            row = onehot(fp >> 4, 16)
            low, high = choose(fp & 15, 16, dot(fl[...], jnp.concatenate([row, row], axis=0)))
            value = jnp.zeros((16, KT), F32)
            for i in range(16):
                y = low[i : i + 1] if i < 8 else high[i - 8 : i - 7]
                value = value + wk[i * 16 : (i + 1) * 16, k] * y
            vs[0, :, k], vs[1, :, k] = split(value)

    turn = lax.div(me, 32) * 16 + lax.rem(me, 16)
    own_half = lax.div(lax.rem(me, 32), 16)

    def send(half, i):
        j = lax.rem(turn + i, 64)
        to = lax.div(j, 16) * 32 + half * 16 + lax.rem(j, 16)
        scatter_one(me, to, z, zr, sems)

    def send_first(half):
        @pl.when(own_half != half)
        def _():
            send(half, 0)

    for half in range(2):
        acc[...] = jnp.zeros_like(acc)

        @pl.loop(0, TILES // 4)
        def _(n):
            if half:
                for i in range(1, 16):
                    send(0, n * 16 + i)

                @pl.when(n > 0)
                def _():
                    send(0, n * 16)
            spreads, slots = [], []
            for u in range(4):
                k = tile_at(n * 4 + u)
                sd, r = sd_ref[:, k], rank[:, k]
                slots.append(onehot((sd >> 5) * 64 + r, 256))
                e = narrow((sd & 31) - half * 16)
                spreads.append(
                    jnp.concatenate([spread_at(e, 16, vs[part, :, k]) for part in range(2)], axis=0)
                )
            acc[...] += dot(jnp.concatenate(spreads, axis=1), jnp.concatenate(slots, axis=1), NT)

        got = acc[0:256] + acc[256:512]
        for t in range(2):
            both = got[:, t * 128 : (t + 1) * 128].reshape(16, 16, 128)
            d = t * 64 + half * 16
            z[d : d + 16], z[d + 32 : d + 48] = swap_halves(both[:, 0:8], both[:, 8:16])

    send_first(0)
    send_first(1)
    for i in range(1, 4):
        send(1, i)

    @pl.loop(1, 16)
    def _(n):
        for i in range(4):
            send(1, n * 4 + i)

    zr[me] = z[me]


def gather_keys(idr, blocks, columns):
    @pl.loop(0, DEV // 16)
    def _(n):
        for u in range(4):
            t = n * 4 + u
            block, column = patch_keys(pick_tags(idr, t * 4))
            blocks[:, tile_at(t)] = narrow(block)
            columns[:, tile_at(t)] = onehot(column, 64)


def gather_up(zr, blocks, columns, acc):
    acc[...] = jnp.zeros_like(acc)

    @pl.loop(0, DEV // 4 // GU)
    def _(n):
        spreads, rows = [], []
        for u in range(GU):
            t = n * GU + u
            s = t * 4
            lows, highs = [], []
            for p in range(2):
                low, high = swap_halves(zr[s + 2 * p], zr[s + 2 * p + 1])
                lows.append(low)
                highs.append(high)
            value = jnp.concatenate(
                [jnp.concatenate(lows, axis=1), jnp.concatenate(highs, axis=1)], axis=0
            )
            block, row = blocks[:, tile_at(t)], columns[:, tile_at(t)]
            for part in split(value):
                spreads.append(spread_at(block, 4, part))
                rows.append(row)
        acc[...] += dot(jnp.concatenate(spreads, axis=1), jnp.concatenate(rows, axis=1), NT)

    return face_of(acc[...]) * FLUX_GAIN


def slope_of(field, index, xlow, xhigh, vel, heat, z):
    centre = field[index]
    rows = lax.broadcasted_iota(I32, (16, 256), 0)
    xbelow = jnp.where(rows == 0, xlow, pltpu.roll(centre, 1, 0))
    xabove = jnp.where(rows == 15, xhigh, pltpu.roll(centre, 15, 0))
    sides = (
        (field[index - 1], field[index + 1]),
        (xbelow, xabove),
        (pltpu.roll(centre, 1, 1), pltpu.roll(centre, 255, 1)),
    )
    total = heat[z].astype(F32)
    for axis, (below, above) in enumerate(sides):
        c = vel[axis, z].astype(F32)
        weight = jnp.maximum(c, 0.0) + DIFFUSION
        total = total + (below - centre) * weight + (above - centre) * (weight - c)
    return centre, total


def predict_block(field, halo, vel, heat, pred, edges, z0, count):
    xlow = halo[0, pl.ds(z0, ZB), :].astype(F32)
    xhigh = halo[1, pl.ds(z0, ZB), :].astype(F32)
    first, last = [], []
    for q in range(count):
        z = z0 + q
        centre, slope = slope_of(
            field, z + 1, xlow[q : q + 1], xhigh[q : q + 1], vel, heat, z
        )
        value = centre + TIMESTEP * slope
        pred[z + 1] = value
        first.append(value[0:1])
        last.append(value[15:16])
    for _ in range(count, ZB):
        first.append(jnp.zeros((1, 256), F32))
        last.append(jnp.zeros((1, 256), F32))
    edges[0, pl.ds(z0, ZB), :] = jnp.concatenate(first, axis=0).astype(BF16)
    edges[1, pl.ds(z0, ZB), :] = jnp.concatenate(last, axis=0).astype(BF16)


def correct_block(pred, halo, vel, heat, field, z0, count):
    xlow = halo[0, pl.ds(z0, ZB), :].astype(F32)
    xhigh = halo[1, pl.ds(z0, ZB), :].astype(F32)
    for q in range(count):
        z = z0 + q
        centre, slope = slope_of(pred, z + 1, xlow[q : q + 1], xhigh[q : q + 1], vel, heat, z)
        field[z + 1] = 0.5 * field[z + 1] + 0.5 * (centre + TIMESTEP * slope)


def widen(own, above, below):
    return jnp.concatenate([own, above, below], axis=own.ndim - 2)


def spread_of(src, z, layers):
    centre = src[z]
    zbelow = src[max(z - 1, 0)]
    zabove = src[z + 1] if z + 1 < layers else jnp.zeros_like(centre)
    total = zbelow + zabove + pltpu.roll(centre, 1, 0) + pltpu.roll(centre, 23, 0)
    return centre, total + pltpu.roll(centre, 1, 1) + pltpu.roll(centre, 255, 1) - 6.0 * centre


def solid_base(solid, cond, halo, s0, s1, cx):
    below = halo[0].astype(F32).reshape(32, 8, 256)
    above = halo[1].astype(F32).reshape(32, 8, 256)
    s0[...] = widen(solid[...], above[:, 0:4], below[:, 0:4])
    cx[...] = CONDUCT_RATE * widen(cond[...], above[:, 4:8], below[:, 4:8])
    src, dst = s0, s1
    for step in range(SUBCYCLES):
        for z in range(32):
            centre, total = spread_of(src, z, 32)
            dst[z] = centre + cx[z] * total
        src, dst = dst, src


def flux_response(wide, cx, t0, t1):
    t0[...] = jnp.zeros_like(t0)
    t1[...] = jnp.zeros_like(t1)
    t0[0] = wide
    src, dst = t0, t1
    for step in range(1, SUBCYCLES):
        for z in range(step + 1):
            centre, total = spread_of(src, z, 5)
            value = centre + cx[z] * total
            dst[z] = value + wide if z == 0 else value
        src, dst = dst, src
    return src


def kernel(
    flow_in, vel_in, heat_in, solid_in, cond_in, table_in, fp, sd, sp, b,
    flow_out, solid_out, rates_out, face_out, face_halo_out,
    field, pred, vel, heat, solid, cond, table, tab, wk, wall, wallt,
    rank, ids, idr, xs, xr, z, zr, lhs, wl,
    fe, fh, pe, ph, pt, pth, se, sh, ff,
    s0, s1, cx, carry, idacc, acc, zacc, vs, blocks, columns,
    insem, outsem, isem, xsem, zsem, psem,
):
    me = lax.axis_index("grp") * 64 + lax.axis_index("dom")
    barrier = pltpu.get_barrier_semaphore()

    loads = [
        pltpu.make_async_copy(src, dst, insem.at[i])
        for i, (src, dst) in enumerate(
            (
                (solid_in, solid),
                (cond_in, cond),
                (flow_in, field.at[pl.ds(1, 128)]),
                (table_in, table),
                (vel_in, vel),
                (heat_in, heat),
            )
        )
    ]
    start_all(loads)

    def greet(n):
        for q in range(32):
            to = peer(me, n * 32 + q)
            if q:
                pl.semaphore_signal(barrier, inc=1, device_id=coords(to), device_id_type=MESH)
            else:

                @pl.when(n > 0)
                def _():
                    pl.semaphore_signal(barrier, inc=1, device_id=coords(to), device_id_type=MESH)

    rank_and_ids(sd, sp, rank, ids, carry, idacc, greet)
    loads[3].wait()
    tab[0], tab[1] = split(table[...])
    loads[0].wait()
    loads[1].wait()
    solid_edges(solid, cond, se)
    loads[2].wait()
    zero = jnp.zeros((16, 256), F32)
    field[0] = zero
    field[129] = zero
    pred[0] = zero
    flow_edges(field, fe)
    pl.semaphore_wait(barrier, DEV - 1)

    scatter_start(me, ids, idr, isem)
    flow_halo = pair_copies(me, fe, fh, psem.at[0])
    solid_halo = pair_copies(me, se, sh, psem.at[1])
    start_all(flow_halo + solid_halo)
    weights(tab, b, wk)

    scatter_wait(idr, isem, 1)
    answers(me, idr, solid, xs, xr, wl, xsem)

    loads[4].wait()
    loads[5].wait()
    wait_all(flow_halo)

    @pl.loop(0, 128 // ZB - 1)
    def _(n):
        predict_block(field, fh, vel, heat, pred, pe, pl.multiple_of(n * ZB, ZB), ZB)

    predict_block(field, fh, vel, heat, pred, pe, 128 - ZB, ZB - 1)
    pred_halo = pair_copies(me, pe, ph, psem.at[2])
    start_all(pred_halo)

    wait_all(solid_halo)
    solid_base(solid, cond, sh, s0, s1, cx)
    rest = pltpu.make_async_copy(s0.at[pl.ds(0, 32), pl.ds(0, 16)], solid_out, outsem.at[8])
    rates = pltpu.make_async_copy(cx.at[pl.ds(0, 4)], rates_out, outsem.at[10])
    rest.start()
    rates.start()

    scatter_wait(xr, xsem, 1)
    forward(xr, fp, sd, rank, wk, lhs, acc, wall)

    field[129] = wall[...]
    pred[129] = wall[...]
    xlow = fh[0, 112:128, :].astype(F32)[15:16]
    xhigh = fh[1, 112:128, :].astype(F32)[15:16]
    centre, slope = slope_of(field, 128, xlow, xhigh, vel, heat, 127)
    top = centre + TIMESTEP * slope
    pred[128] = top
    pt[0] = top[0:1]
    pt[1] = top[15:16]
    top_halo = pair_copies(me, pt, pth, psem.at[3])
    start_all(top_halo)

    wait_all(pred_halo)

    def correct(n):
        z0 = pl.multiple_of(n * ZB, ZB)
        correct_block(pred, ph, vel, heat, field, z0, ZB)
        out = pl.ds(z0, ZB)
        pltpu.make_async_copy(field.at[pl.ds(z0 + 1, ZB)], flow_out.at[out], outsem.at[n]).start()

    @pl.loop(0, C_FIRST)
    def _(n):
        correct(n)

    wait_all(top_halo)
    centre, slope = slope_of(pred, 128, pth[0], pth[1], vel, heat, 127)
    done = 0.5 * field[128] + 0.5 * (centre + TIMESTEP * slope)
    field[128] = done
    flux = FILM_COEFF * (done - wall[...])
    backward(me, flux, wk, fp, sd, rank, wl, vs, zacc, z, zr, zsem)

    @pl.loop(C_FIRST, 128 // ZB - 1)
    def _(n):
        correct(n)

    correct_block(pred, ph, vel, heat, field, 128 - ZB, ZB - 1)
    last = 128 // ZB - 1
    pltpu.make_async_copy(
        field.at[pl.ds(129 - ZB, ZB)], flow_out.at[pl.ds(128 - ZB, ZB)], outsem.at[last]
    ).start()

    gather_keys(idr, blocks, columns)
    scatter_wait(zr, zsem, 1)
    total = gather_up(zr, blocks, columns, acc)
    ff[0] = total[0:4]
    ff[1] = total[12:16]
    face_halo = pair_copies(me, ff, face_halo_out, psem.at[4])
    start_all(face_halo)
    wallt[...] = total
    near = pltpu.make_async_copy(wallt, face_out, outsem.at[9])
    near.start()

    @pl.loop(0, 128 // ZB)
    def _(n):
        out = pl.ds(pl.multiple_of(n * ZB, ZB), ZB)
        pltpu.make_async_copy(field.at[pl.ds(n * ZB + 1, ZB)], flow_out.at[out], outsem.at[n]).wait()

    scatter_wait(ids, isem, 0)
    scatter_wait(xs, xsem, 0)
    scatter_wait(z, zsem, 0)
    rest.wait()
    rates.wait()
    near.wait()
    wait_all(face_halo)


C_FIRST = 6
FU = 8
BU = 8
GU = 16
CODE = 32767.0 / 6.0


def finish_kernel(
    flow_in, solid_in, rates_in, face_in, halo_in,
    flow_out, solid_out,
    flow, solid, rates, face, halo, t0, t1, insem, outsem,
):
    small = [
        pltpu.make_async_copy(src, dst, insem.at[8 + i])
        for i, (src, dst) in enumerate(
            ((face_in, face), (halo_in, halo), (rates_in, rates), (solid_in, solid))
        )
    ]
    first, second = [], []
    for n in range(8):
        part = pl.ds(n * 16, 16)
        first.append(pltpu.make_async_copy(flow_in.at[part], flow.at[part], insem.at[n]))
        second.append(pltpu.make_async_copy(flow.at[part], flow_out.at[part], outsem.at[n]))
    start_all(small)
    start_all(first)
    wait_all(small)
    far = pltpu.make_async_copy(solid.at[pl.ds(4, 28)], solid_out.at[pl.ds(4, 28)], outsem.at[8])
    far.start()
    for n in range(6):
        first[n].wait()
        second[n].start()
    response = flux_response(widen(face[...], halo[1], halo[0]), rates, t0, t1)
    solid[0:4] = solid[0:4] + response[0:4, 0:16, :]
    near = pltpu.make_async_copy(solid.at[pl.ds(0, 4)], solid_out.at[pl.ds(0, 4)], outsem.at[9])
    near.start()
    for n in range(6, 8):
        first[n].wait()
        second[n].start()
    wait_all(second)
    far.wait()
    near.wait()


def finish(*parts):
    hbm = pl.BlockSpec(memory_space=pl.ANY)
    return pl.pallas_call(
        finish_kernel,
        out_shape=(
            jax.ShapeDtypeStruct((128, 16, 256), F32),
            jax.ShapeDtypeStruct((32, 16, 256), F32),
        ),
        in_specs=[hbm] * 5,
        out_specs=(hbm, hbm),
        scratch_shapes=[
            pltpu.VMEM((128, 16, 256), F32),
            pltpu.VMEM((32, 16, 256), F32),
            pltpu.VMEM((4, 24, 256), F32),
            pltpu.VMEM((16, 256), F32),
            pltpu.VMEM((2, 4, 256), F32),
            pltpu.VMEM((5, 24, 256), F32),
            pltpu.VMEM((5, 24, 256), F32),
            pltpu.SemaphoreType.DMA((12,)),
            pltpu.SemaphoreType.DMA((10,)),
        ],
        compiler_params=pltpu.CompilerParams(vmem_limit_bytes=60 * 1024 * 1024),
        name="finish",
    )(*parts)


def body(flow, vel, heat, solid, cond, table, fp, sd, sp, b):
    fp, sd, sp, b = (v.reshape(1, NK) for v in (fp, sd, sp, b))
    vm, hbm = pl.BlockSpec(memory_space=pltpu.VMEM), pl.BlockSpec(memory_space=pl.ANY)
    dma = pltpu.SemaphoreType.DMA
    scratch = [
        pltpu.VMEM((130, 16, 256), F32),
        pltpu.VMEM((130, 16, 256), F32),
        pltpu.VMEM((3, 128, 16, 256), BF16),
        pltpu.VMEM((128, 16, 256), BF16),
        pltpu.VMEM((32, 16, 256), F32),
        pltpu.VMEM((32, 16, 256), F32),
        pltpu.VMEM((256, 1024), F32),
        pltpu.VMEM((2, 256, 1024), BF16),
        pltpu.VMEM((256, NK), F32),
        pltpu.VMEM((16, 256), F32),
        pltpu.VMEM((16, 256), F32),
        pltpu.VMEM((1, NK), I32),
        pltpu.VMEM((DEV, 1, 128), F32),
        pltpu.VMEM((DEV, 1, 128), F32),
        pltpu.VMEM((DEV, 8, 128), I16),
        pltpu.VMEM((DEV, 8, 128), I16),
        pltpu.VMEM((DEV, 8, 128), F32),
        pltpu.VMEM((DEV, 8, 128), F32),
        pltpu.VMEM((512, 512), BF16),
        pltpu.VMEM((256, 32), BF16),
        pltpu.VMEM((2, 128, 256), BF16),
        pltpu.VMEM((2, 128, 256), BF16),
        pltpu.VMEM((2, 128, 256), BF16),
        pltpu.VMEM((2, 128, 256), BF16),
        pltpu.VMEM((2, 1, 256), F32),
        pltpu.VMEM((2, 1, 256), F32),
        pltpu.VMEM((2, 16, 16, 256), BF16),
        pltpu.VMEM((2, 16, 16, 256), BF16),
        pltpu.VMEM((2, 4, 256), F32),
        pltpu.VMEM((32, 24, 256), F32),
        pltpu.VMEM((32, 24, 256), F32),
        pltpu.VMEM((32, 24, 256), F32),
        pltpu.VMEM((DEV, KT), F32),
        pltpu.VMEM((32, 256), F32),
        pltpu.VMEM((64, 64), F32),
        pltpu.VMEM((512, 256), F32),
        pltpu.VMEM((2, 16, NK), BF16),
        pltpu.VMEM((16, 2 * NK), I16),
        pltpu.VMEM((64, 2 * NK), BF16),
        dma((6,)),
        dma((11,)),
        dma((2,)),
        dma((2,)),
        dma((2,)),
        dma((5, 4)),
    ]
    results = pl.pallas_call(
        kernel,
        out_shape=(
            jax.ShapeDtypeStruct((128, 16, 256), F32),
            jax.ShapeDtypeStruct((32, 16, 256), F32),
            jax.ShapeDtypeStruct((4, 24, 256), F32),
            jax.ShapeDtypeStruct((16, 256), F32),
            jax.ShapeDtypeStruct((2, 4, 256), F32),
        ),
        in_specs=[hbm] * 6 + [vm] * 4,
        out_specs=(hbm,) * 5,
        scratch_shapes=scratch,
        compiler_params=pltpu.CompilerParams(
            vmem_limit_bytes=60 * 1024 * 1024, collective_id=0, has_side_effects=True
        ),
        name="coupled",
    )(flow, vel, heat, solid, cond, table.reshape(256, 1024), fp, sd, sp, b)
    return finish(*results)


def solution(mesh):
    placed = (
        P(None, ("grp", "dom"), None),
        P(None, None, ("grp", "dom"), None),
        P(None, ("grp", "dom"), None),
        P(None, ("grp", "dom"), None),
        P(None, ("grp", "dom"), None),
        P(),
        P(("grp", "dom")),
        P(("grp", "dom"), None),
        P(("grp", "dom")),
        P(("grp", "dom")),
    )
    return jax.shard_map(
        body,
        mesh=mesh,
        in_specs=placed,
        out_specs=(P(None, ("grp", "dom"), None), P(None, ("grp", "dom"), None)),
        check_vma=False,
    )
```

```python
import jax
import jax.numpy as jnp
from jax import lax
from jax.experimental import pallas as pl
from jax.experimental.pallas import tpu as pltpu
from jax.sharding import PartitionSpec as P

MESH = pl.DeviceIdType.MESH
F32, BF16, I32, I16 = jnp.float32, jnp.bfloat16, jnp.int32, jnp.int16

SUBCYCLES = 4
DIFFUSION = 0.8
TIMESTEP = 0.12
FILM_COEFF = 1.0
CONDUCT_RATE = 0.08
FLUX_GAIN = 0.25

DEV = 128
KT = 256
NK = 4096
TILES = NK // KT
ZB = 16
NN = (((1,), (0,)), ((), ()))
NT = (((1,), (1,)), ((), ()))


def dot(a, b, dims=NN):
    return lax.dot_general(a, b, dims, preferred_element_type=F32)


def narrow(row):
    return jnp.broadcast_to(row, (16, row.shape[1])).astype(I16)


def onehot(row, rows):
    key = narrow(row)
    place = lax.broadcasted_iota(I32, key.shape, 0).astype(I16)
    one, zero = BF16(1), BF16(0)
    return jnp.concatenate(
        [jnp.where(place == key - I16(16 * v), one, zero) for v in range(rows // 16)], axis=0
    )


def spread(key, count, value):
    return spread_at(narrow(key), count, value)


def spread_at(key, count, value):
    return jnp.concatenate([jnp.where(key == I16(v), value, BF16(0)) for v in range(count)], axis=0)


def patch_keys(patch):
    return (patch >> 2) & 3, (patch & 3) * 16 + (patch >> 4)


def face_of(sums):
    turned = sums.T
    return jnp.concatenate(
        [
            turned[c % 4 * 16 : c % 4 * 16 + 16, c // 4 * 16 : c // 4 * 16 + 16]
            for c in range(16)
        ],
        axis=1,
    )


def choose(key, count, blocks):
    key = jnp.broadcast_to(key, (8, key.shape[1]))
    low = high = jnp.zeros(key.shape, F32)
    for v in range(count):
        mask = key == v
        low = jnp.where(mask, blocks[v * 16 : v * 16 + 8], low)
        high = jnp.where(mask, blocks[v * 16 + 8 : v * 16 + 16], high)
    return low, high


def split(value):
    high = value.astype(BF16)
    return high, (value - high.astype(F32)).astype(BF16)


def beside(value):
    high, low = split(value.T)
    return jnp.concatenate([high, low], axis=1)


def swap_halves(low, high):
    axis = low.ndim - 1
    left = lax.broadcasted_iota(I32, low.shape, axis) < 64
    return jnp.where(left, low, pltpu.roll(high, 64, axis)), jnp.where(
        left, pltpu.roll(low, 64, axis), high
    )


def encode(value):
    step = jnp.floor(jnp.clip(value * CODE, -32767.0, 32767.0) + 0.5)
    return step.astype(I32).astype(I16)


def tile_at(t, size=KT):
    return pl.ds(pl.multiple_of(t * size, size), size)


def coords(device):
    return (lax.div(device, 64), lax.rem(device, 64))


def peer(me, offset):
    return lax.rem(me + offset, DEV)


def remote(src, dst, send, recv, device):
    return pltpu.make_async_remote_copy(
        src_ref=src,
        dst_ref=dst,
        send_sem=send,
        recv_sem=recv,
        device_id=coords(device),
        device_id_type=MESH,
    )


def pair_copies(me, edges, halo, sems):
    up = remote(edges.at[1], halo.at[0], sems.at[0], sems.at[1], peer(me, 1))
    down = remote(edges.at[0], halo.at[1], sems.at[2], sems.at[3], peer(me, DEV - 1))
    return up, down


def start_all(copies):
    for copy in copies:
        copy.start()


def wait_all(copies):
    for copy in copies:
        copy.wait()


def scatter_one(me, to, src, dst, sems):
    remote(src.at[to], dst.at[me], sems.at[0], sems.at[1], to).start()


def scatter_start(me, src, dst, sems):
    for o in range(1, 8):
        scatter_one(me, peer(me, o), src, dst, sems)

    @pl.loop(1, DEV // 8)
    def _(n):
        for q in range(8):
            scatter_one(me, peer(me, n * 8 + q), src, dst, sems)

    dst[me] = src[me]


def scatter_wait(ref, sems, which):
    many = ref.at[pl.ds(0, DEV - 1)]
    pltpu.make_async_copy(many, many, sems.at[which]).wait()


def rank_and_ids(sd_ref, sp_ref, rank, ids, carry, acc, beside_it):
    before = lax.broadcasted_iota(I32, (KT, KT), 0) < lax.broadcasted_iota(I32, (KT, KT), 1)
    before = jnp.where(before, 1.0, 0.0).astype(BF16)
    every = jnp.ones((KT, KT), BF16)
    carry[...] = jnp.zeros_like(carry)
    acc[...] = jnp.zeros_like(acc)

    @pl.loop(0, TILES // 4)
    def _(n):
        beside_it(n)
        held, total = carry[...], jnp.zeros((32, 256), F32)
        for u in range(4):
            k = tile_at(n * 4 + u)
            sd = sd_ref[:, k]
            mine = lax.broadcasted_iota(I32, (DEV, KT), 0) == sd
            one = onehot(sd, DEV)
            ahead = dot(one, before) + held
            r = jnp.sum(jnp.where(mine, ahead, 0.0), axis=0, keepdims=True).astype(I32)
            held = held + dot(one, every)
            rank[:, k] = r
            tag = (sp_ref[:, k] + 1).astype(F32)
            place = lax.broadcasted_iota(I32, (32, KT), 0)
            m = jnp.where(place == (sd & 31), tag, 0.0).astype(BF16)
            total = total + dot(m, onehot((sd >> 5) * 64 + r, 256), NT)
        carry[...] = held
        acc[...] += total

    got = acc[...]
    left = lax.broadcasted_iota(I32, (32, 128), 1) < 64
    for t in range(2):
        both = got[:, t * 128 : (t + 1) * 128]
        turned = pltpu.roll(both, 64, 1)
        ids[t * 64 : t * 64 + 32] = jnp.where(left, both, turned).reshape(32, 1, 128)
        ids[t * 64 + 32 : t * 64 + 64] = jnp.where(left, turned, both).reshape(32, 1, 128)


def flow_edges(field, edges):
    @pl.loop(0, 128 // ZB)
    def _(b):
        z0 = pl.multiple_of(b * ZB, ZB)
        block = field[pl.ds(z0 + 1, ZB)]
        edges[0, pl.ds(z0, ZB), :] = block[:, 0, :].astype(BF16)
        edges[1, pl.ds(z0, ZB), :] = block[:, 15, :].astype(BF16)


def solid_edges(solid, cond, edges):
    low = jnp.concatenate([solid[:, 0:4, :], cond[:, 0:4, :]], axis=1)
    high = jnp.concatenate([solid[:, 12:16, :], cond[:, 12:16, :]], axis=1)
    edges[0] = low.reshape(16, 16, 256).astype(BF16)
    edges[1] = high.reshape(16, 16, 256).astype(BF16)


def pick_tags(idr, s):
    left = lax.broadcasted_iota(I32, (1, 128), 1) < 64
    pairs = [jnp.where(left, idr[s + 2 * p], idr[s + 2 * p + 1]) for p in range(2)]
    return jnp.concatenate(pairs, axis=1).astype(I32) - 1


def answers(me, idr, solid, xs, xr, wl, sems):
    wl[...] = beside(solid[0])
    first, turn = lax.div(me, 16), lax.rem(me, 16)

    def send(n, q):
        to = lax.rem(first + n, 8) * 16 + lax.rem(turn + q, 16)
        scatter_one(me, to, xs, xr, sems)

    def group(n):
        base = lax.rem(first + n, 8) * 16
        for u in range(4):
            s = base + u * 4
            tag = pick_tags(idr, s)
            row = onehot(tag >> 4, 16)
            blocks = dot(wl[...], jnp.concatenate([row, row], axis=0))
            low, high = choose(tag & 15, 16, blocks)
            for p in range(2):
                lanes = slice(p * 128, (p + 1) * 128)
                one, two = swap_halves(low[:, lanes], high[:, lanes])
                xs[s + 2 * p] = encode(one)
                xs[s + 2 * p + 1] = encode(two)

    group(0)
    for q in range(1, 16):
        send(0, q)
    group(1)

    @pl.loop(1, 7)
    def _(n):
        for q in range(16):
            send(n, q)
        group(n + 1)

    for q in range(16):
        send(7, q)
    xr[me] = xs[me]


def weights(tab, b_ref, wk):
    @pl.loop(0, TILES // 2)
    def _(n):
        for u in range(2):
            k = tile_at(n * 2 + u)
            block = onehot(b_ref[:, k], 1024)
            wk[:, k] = dot(tab[0], block) + dot(tab[1], block)


def forward(xr, fp_ref, sd_ref, rank, wk, lhs, acc, face):
    for t in range(2):
        d = t * 64
        one = xr[d : d + 32].astype(I32).astype(F32)
        two = xr[d + 32 : d + 64].astype(I32).astype(F32)
        both = jnp.concatenate(swap_halves(one, two), axis=1).reshape(512, 128)
        high, low = split(both)
        lhs[:, t * 128 : (t + 1) * 128] = high
        lhs[:, 256 + t * 128 : 256 + (t + 1) * 128] = low
    acc[...] = jnp.zeros_like(acc)

    @pl.loop(0, TILES // FU)
    def _(n):
        spreads, rows = [], []
        for u in range(FU):
            k = tile_at(n * FU + u)
            fp, sd, r = fp_ref[:, k], sd_ref[:, k], rank[:, k]
            slot = onehot((sd >> 5) * 64 + r, 256)
            blocks = dot(lhs[...], jnp.concatenate([slot, slot], axis=0))
            low, high = choose(sd & 31, 32, blocks)
            w = wk[:, k]
            y = jnp.concatenate(
                [
                    jnp.sum(
                        w[i * 16 : i * 16 + 8] * low + w[i * 16 + 8 : i * 16 + 16] * high,
                        axis=0,
                        keepdims=True,
                    )
                    for i in range(16)
                ],
                axis=0,
            )
            block, column = patch_keys(fp)
            block, row = narrow(block), onehot(column, 64)
            for part in split(y * (1.0 / CODE)):
                spreads.append(spread_at(block, 4, part))
                rows.append(row)
        acc[...] += dot(jnp.concatenate(spreads, axis=1), jnp.concatenate(rows, axis=1), NT)

    face[...] = face_of(acc[...])


def backward(me, flux, wk, fp_ref, sd_ref, rank, fl, vs, acc, z, zr, sems):
    fl[...] = beside(flux)

    @pl.loop(0, TILES // BU)
    def _(n):
        for u in range(BU):
            k = tile_at(n * BU + u)
            fp = fp_ref[:, k]
            row = onehot(fp >> 4, 16)
            low, high = choose(fp & 15, 16, dot(fl[...], jnp.concatenate([row, row], axis=0)))
            value = jnp.zeros((16, KT), F32)
            for i in range(16):
                y = low[i : i + 1] if i < 8 else high[i - 8 : i - 7]
                value = value + wk[i * 16 : (i + 1) * 16, k] * y
            vs[0, :, k], vs[1, :, k] = split(value)

    turn = lax.div(me, 32) * 16 + lax.rem(me, 16)
    own_half = lax.div(lax.rem(me, 32), 16)

    def send(half, i):
        j = lax.rem(turn + i, 64)
        to = lax.div(j, 16) * 32 + half * 16 + lax.rem(j, 16)
        scatter_one(me, to, z, zr, sems)

    def send_first(half):
        @pl.when(own_half != half)
        def _():
            send(half, 0)

    for half in range(2):
        acc[...] = jnp.zeros_like(acc)

        @pl.loop(0, TILES // 4)
        def _(n):
            if half:
                for i in range(1, 16):
                    send(0, n * 16 + i)

                @pl.when(n > 0)
                def _():
                    send(0, n * 16)
            spreads, slots = [], []
            for u in range(4):
                k = tile_at(n * 4 + u)
                sd, r = sd_ref[:, k], rank[:, k]
                slots.append(onehot((sd >> 5) * 64 + r, 256))
                e = narrow((sd & 31) - half * 16)
                spreads.append(
                    jnp.concatenate([spread_at(e, 16, vs[part, :, k]) for part in range(2)], axis=0)
                )
            acc[...] += dot(jnp.concatenate(spreads, axis=1), jnp.concatenate(slots, axis=1), NT)

        got = acc[0:256] + acc[256:512]
        for t in range(2):
            both = got[:, t * 128 : (t + 1) * 128].reshape(16, 16, 128)
            d = t * 64 + half * 16
            z[d : d + 16], z[d + 32 : d + 48] = swap_halves(both[:, 0:8], both[:, 8:16])

    send_first(0)
    send_first(1)
    for i in range(1, 4):
        send(1, i)

    @pl.loop(1, 16)
    def _(n):
        for i in range(4):
            send(1, n * 4 + i)

    zr[me] = z[me]


def gather_keys(idr, blocks, columns):
    @pl.loop(0, DEV // 16)
    def _(n):
        for u in range(4):
            t = n * 4 + u
            block, column = patch_keys(pick_tags(idr, t * 4))
            blocks[:, tile_at(t)] = narrow(block)
            columns[:, tile_at(t)] = onehot(column, 64)


def gather_up(zr, blocks, columns, acc):
    acc[...] = jnp.zeros_like(acc)

    @pl.loop(0, DEV // 4 // GU)
    def _(n):
        spreads, rows = [], []
        for u in range(GU):
            t = n * GU + u
            s = t * 4
            lows, highs = [], []
            for p in range(2):
                low, high = swap_halves(zr[s + 2 * p], zr[s + 2 * p + 1])
                lows.append(low)
                highs.append(high)
            value = jnp.concatenate(
                [jnp.concatenate(lows, axis=1), jnp.concatenate(highs, axis=1)], axis=0
            )
            block, row = blocks[:, tile_at(t)], columns[:, tile_at(t)]
            for part in split(value):
                spreads.append(spread_at(block, 4, part))
                rows.append(row)
        acc[...] += dot(jnp.concatenate(spreads, axis=1), jnp.concatenate(rows, axis=1), NT)

    return face_of(acc[...]) * FLUX_GAIN


def slope_of(field, index, xlow, xhigh, vel, heat, z):
    centre = field[index]
    rows = lax.broadcasted_iota(I32, (16, 256), 0)
    xbelow = jnp.where(rows == 0, xlow, pltpu.roll(centre, 1, 0))
    xabove = jnp.where(rows == 15, xhigh, pltpu.roll(centre, 15, 0))
    sides = (
        (field[index - 1], field[index + 1]),
        (xbelow, xabove),
        (pltpu.roll(centre, 1, 1), pltpu.roll(centre, 255, 1)),
    )
    total = heat[z].astype(F32)
    for axis, (below, above) in enumerate(sides):
        c = vel[axis, z].astype(F32)
        weight = jnp.maximum(c, 0.0) + DIFFUSION
        total = total + (below - centre) * weight + (above - centre) * (weight - c)
    return centre, total


def predict_block(field, halo, vel, heat, pred, edges, z0, count):
    xlow = halo[0, pl.ds(z0, ZB), :].astype(F32)
    xhigh = halo[1, pl.ds(z0, ZB), :].astype(F32)
    first, last = [], []
    for q in range(count):
        z = z0 + q
        centre, slope = slope_of(
            field, z + 1, xlow[q : q + 1], xhigh[q : q + 1], vel, heat, z
        )
        value = centre + TIMESTEP * slope
        pred[z + 1] = value
        first.append(value[0:1])
        last.append(value[15:16])
    for _ in range(count, ZB):
        first.append(jnp.zeros((1, 256), F32))
        last.append(jnp.zeros((1, 256), F32))
    edges[0, pl.ds(z0, ZB), :] = jnp.concatenate(first, axis=0).astype(BF16)
    edges[1, pl.ds(z0, ZB), :] = jnp.concatenate(last, axis=0).astype(BF16)


def correct_block(pred, halo, vel, heat, field, z0, count):
    xlow = halo[0, pl.ds(z0, ZB), :].astype(F32)
    xhigh = halo[1, pl.ds(z0, ZB), :].astype(F32)
    for q in range(count):
        z = z0 + q
        centre, slope = slope_of(pred, z + 1, xlow[q : q + 1], xhigh[q : q + 1], vel, heat, z)
        field[z + 1] = 0.5 * field[z + 1] + 0.5 * (centre + TIMESTEP * slope)


def widen(own, above, below):
    return jnp.concatenate([own, above, below], axis=own.ndim - 2)


def spread_of(src, z, layers):
    centre = src[z]
    zbelow = src[max(z - 1, 0)]
    zabove = src[z + 1] if z + 1 < layers else jnp.zeros_like(centre)
    total = zbelow + zabove + pltpu.roll(centre, 1, 0) + pltpu.roll(centre, 23, 0)
    return centre, total + pltpu.roll(centre, 1, 1) + pltpu.roll(centre, 255, 1) - 6.0 * centre


def solid_base(solid, cond, halo, s0, s1, cx):
    below = halo[0].astype(F32).reshape(32, 8, 256)
    above = halo[1].astype(F32).reshape(32, 8, 256)
    s0[...] = widen(solid[...], above[:, 0:4], below[:, 0:4])
    cx[...] = CONDUCT_RATE * widen(cond[...], above[:, 4:8], below[:, 4:8])
    src, dst = s0, s1
    for step in range(SUBCYCLES):
        for z in range(32):
            centre, total = spread_of(src, z, 32)
            dst[z] = centre + cx[z] * total
        src, dst = dst, src


def flux_response(wide, cx, t0, t1):
    t0[...] = jnp.zeros_like(t0)
    t1[...] = jnp.zeros_like(t1)
    t0[0] = wide
    src, dst = t0, t1
    for step in range(1, SUBCYCLES):
        for z in range(step + 1):
            centre, total = spread_of(src, z, 5)
            value = centre + cx[z] * total
            dst[z] = value + wide if z == 0 else value
        src, dst = dst, src
    return src


def kernel(
    flow_in, vel_in, heat_in, solid_in, cond_in, table_in, fp, sd, sp, b,
    flow_out, solid_out, rates_out, face_out, face_halo_out,
    field, pred, vel, heat, solid, cond, table, tab, wk, wall, wallt,
    rank, ids, idr, xs, xr, z, zr, lhs, wl,
    fe, fh, pe, ph, pt, pth, se, sh, ff,
    s0, s1, cx, carry, idacc, acc, zacc, vs, blocks, columns,
    insem, outsem, isem, xsem, zsem, psem,
):
    me = lax.axis_index("grp") * 64 + lax.axis_index("dom")
    barrier = pltpu.get_barrier_semaphore()

    loads = [
        pltpu.make_async_copy(src, dst, insem.at[i])
        for i, (src, dst) in enumerate(
            (
                (solid_in, solid),
                (cond_in, cond),
                (flow_in, field.at[pl.ds(1, 128)]),
                (table_in, table),
                (vel_in, vel),
                (heat_in, heat),
            )
        )
    ]
    start_all(loads)

    def greet(n):
        for q in range(32):
            to = peer(me, n * 32 + q)
            if q:
                pl.semaphore_signal(barrier, inc=1, device_id=coords(to), device_id_type=MESH)
            else:

                @pl.when(n > 0)
                def _():
                    pl.semaphore_signal(barrier, inc=1, device_id=coords(to), device_id_type=MESH)

    rank_and_ids(sd, sp, rank, ids, carry, idacc, greet)
    loads[3].wait()
    tab[0], tab[1] = split(table[...])
    loads[0].wait()
    loads[1].wait()
    solid_edges(solid, cond, se)
    loads[2].wait()
    zero = jnp.zeros((16, 256), F32)
    field[0] = zero
    field[129] = zero
    pred[0] = zero
    flow_edges(field, fe)
    pl.semaphore_wait(barrier, DEV - 1)

    scatter_start(me, ids, idr, isem)
    flow_halo = pair_copies(me, fe, fh, psem.at[0])
    solid_halo = pair_copies(me, se, sh, psem.at[1])
    start_all(flow_halo + solid_halo)
    weights(tab, b, wk)

    scatter_wait(idr, isem, 1)
    answers(me, idr, solid, xs, xr, wl, xsem)

    loads[4].wait()
    loads[5].wait()
    wait_all(flow_halo)

    @pl.loop(0, 128 // ZB - 1)
    def _(n):
        predict_block(field, fh, vel, heat, pred, pe, pl.multiple_of(n * ZB, ZB), ZB)

    predict_block(field, fh, vel, heat, pred, pe, 128 - ZB, ZB - 1)
    pred_halo = pair_copies(me, pe, ph, psem.at[2])
    start_all(pred_halo)

    wait_all(solid_halo)
    solid_base(solid, cond, sh, s0, s1, cx)
    rest = pltpu.make_async_copy(s0.at[pl.ds(0, 32), pl.ds(0, 16)], solid_out, outsem.at[8])
    rates = pltpu.make_async_copy(cx.at[pl.ds(0, 4)], rates_out, outsem.at[10])
    rest.start()
    rates.start()

    scatter_wait(xr, xsem, 1)
    forward(xr, fp, sd, rank, wk, lhs, acc, wall)

    field[129] = wall[...]
    pred[129] = wall[...]
    xlow = fh[0, 112:128, :].astype(F32)[15:16]
    xhigh = fh[1, 112:128, :].astype(F32)[15:16]
    centre, slope = slope_of(field, 128, xlow, xhigh, vel, heat, 127)
    top = centre + TIMESTEP * slope
    pred[128] = top
    pt[0] = top[0:1]
    pt[1] = top[15:16]
    top_halo = pair_copies(me, pt, pth, psem.at[3])
    start_all(top_halo)

    wait_all(pred_halo)

    def correct(n):
        z0 = pl.multiple_of(n * ZB, ZB)
        correct_block(pred, ph, vel, heat, field, z0, ZB)
        out = pl.ds(z0, ZB)
        pltpu.make_async_copy(field.at[pl.ds(z0 + 1, ZB)], flow_out.at[out], outsem.at[n]).start()

    @pl.loop(0, C_FIRST)
    def _(n):
        correct(n)

    wait_all(top_halo)
    centre, slope = slope_of(pred, 128, pth[0], pth[1], vel, heat, 127)
    done = 0.5 * field[128] + 0.5 * (centre + TIMESTEP * slope)
    field[128] = done
    flux = FILM_COEFF * (done - wall[...])
    backward(me, flux, wk, fp, sd, rank, wl, vs, zacc, z, zr, zsem)

    @pl.loop(C_FIRST, 128 // ZB - 1)
    def _(n):
        correct(n)

    correct_block(pred, ph, vel, heat, field, 128 - ZB, ZB - 1)
    last = 128 // ZB - 1
    pltpu.make_async_copy(
        field.at[pl.ds(129 - ZB, ZB)], flow_out.at[pl.ds(128 - ZB, ZB)], outsem.at[last]
    ).start()

    gather_keys(idr, blocks, columns)
    scatter_wait(zr, zsem, 1)
    total = gather_up(zr, blocks, columns, acc)
    ff[0] = total[0:4]
    ff[1] = total[12:16]
    face_halo = pair_copies(me, ff, face_halo_out, psem.at[4])
    start_all(face_halo)
    wallt[...] = total
    near = pltpu.make_async_copy(wallt, face_out, outsem.at[9])
    near.start()

    @pl.loop(0, 128 // ZB)
    def _(n):
        out = pl.ds(pl.multiple_of(n * ZB, ZB), ZB)
        pltpu.make_async_copy(field.at[pl.ds(n * ZB + 1, ZB)], flow_out.at[out], outsem.at[n]).wait()

    scatter_wait(ids, isem, 0)
    scatter_wait(xs, xsem, 0)
    scatter_wait(z, zsem, 0)
    rest.wait()
    rates.wait()
    near.wait()
    wait_all(face_halo)


C_FIRST = 6
FU = 8
BU = 8
GU = 16
CODE = 32767.0 / 6.0


def finish_kernel(
    flow_in, solid_in, rates_in, face_in, halo_in,
    flow_out, solid_out,
    flow, solid, rates, face, halo, t0, t1, insem, outsem,
):
    small = [
        pltpu.make_async_copy(src, dst, insem.at[8 + i])
        for i, (src, dst) in enumerate(
            ((face_in, face), (halo_in, halo), (rates_in, rates), (solid_in, solid))
        )
    ]
    first, second = [], []
    for n in range(8):
        part = pl.ds(n * 16, 16)
        first.append(pltpu.make_async_copy(flow_in.at[part], flow.at[part], insem.at[n]))
        second.append(pltpu.make_async_copy(flow.at[part], flow_out.at[part], outsem.at[n]))
    start_all(small)
    start_all(first)
    wait_all(small)
    far = pltpu.make_async_copy(solid.at[pl.ds(4, 28)], solid_out.at[pl.ds(4, 28)], outsem.at[8])
    far.start()
    for n in range(6):
        first[n].wait()
        second[n].start()
    response = flux_response(widen(face[...], halo[1], halo[0]), rates, t0, t1)
    solid[0:4] = solid[0:4] + response[0:4, 0:16, :]
    near = pltpu.make_async_copy(solid.at[pl.ds(0, 4)], solid_out.at[pl.ds(0, 4)], outsem.at[9])
    near.start()
    for n in range(6, 8):
        first[n].wait()
        second[n].start()
    wait_all(second)
    far.wait()
    near.wait()


def finish(*parts):
    hbm = pl.BlockSpec(memory_space=pl.ANY)
    return pl.pallas_call(
        finish_kernel,
        out_shape=(
            jax.ShapeDtypeStruct((128, 16, 256), F32),
            jax.ShapeDtypeStruct((32, 16, 256), F32),
        ),
        in_specs=[hbm] * 5,
        out_specs=(hbm, hbm),
        scratch_shapes=[
            pltpu.VMEM((128, 16, 256), F32),
            pltpu.VMEM((32, 16, 256), F32),
            pltpu.VMEM((4, 24, 256), F32),
            pltpu.VMEM((16, 256), F32),
            pltpu.VMEM((2, 4, 256), F32),
            pltpu.VMEM((5, 24, 256), F32),
            pltpu.VMEM((5, 24, 256), F32),
            pltpu.SemaphoreType.DMA((12,)),
            pltpu.SemaphoreType.DMA((10,)),
        ],
        compiler_params=pltpu.CompilerParams(vmem_limit_bytes=60 * 1024 * 1024),
        name="finish",
    )(*parts)


def body(flow, vel, heat, solid, cond, table, fp, sd, sp, b):
    fp, sd, sp, b = (v.reshape(1, NK) for v in (fp, sd, sp, b))
    vm, hbm = pl.BlockSpec(memory_space=pltpu.VMEM), pl.BlockSpec(memory_space=pl.ANY)
    dma = pltpu.SemaphoreType.DMA
    scratch = [
        pltpu.VMEM((130, 16, 256), F32),
        pltpu.VMEM((130, 16, 256), F32),
        pltpu.VMEM((3, 128, 16, 256), BF16),
        pltpu.VMEM((128, 16, 256), BF16),
        pltpu.VMEM((32, 16, 256), F32),
        pltpu.VMEM((32, 16, 256), F32),
        pltpu.VMEM((256, 1024), F32),
        pltpu.VMEM((2, 256, 1024), BF16),
        pltpu.VMEM((256, NK), F32),
        pltpu.VMEM((16, 256), F32),
        pltpu.VMEM((16, 256), F32),
        pltpu.VMEM((1, NK), I32),
        pltpu.VMEM((DEV, 1, 128), F32),
        pltpu.VMEM((DEV, 1, 128), F32),
        pltpu.VMEM((DEV, 8, 128), I16),
        pltpu.VMEM((DEV, 8, 128), I16),
        pltpu.VMEM((DEV, 8, 128), F32),
        pltpu.VMEM((DEV, 8, 128), F32),
        pltpu.VMEM((512, 512), BF16),
        pltpu.VMEM((256, 32), BF16),
        pltpu.VMEM((2, 128, 256), BF16),
        pltpu.VMEM((2, 128, 256), BF16),
        pltpu.VMEM((2, 128, 256), BF16),
        pltpu.VMEM((2, 128, 256), BF16),
        pltpu.VMEM((2, 1, 256), F32),
        pltpu.VMEM((2, 1, 256), F32),
        pltpu.VMEM((2, 16, 16, 256), BF16),
        pltpu.VMEM((2, 16, 16, 256), BF16),
        pltpu.VMEM((2, 4, 256), F32),
        pltpu.VMEM((32, 24, 256), F32),
        pltpu.VMEM((32, 24, 256), F32),
        pltpu.VMEM((32, 24, 256), F32),
        pltpu.VMEM((DEV, KT), F32),
        pltpu.VMEM((32, 256), F32),
        pltpu.VMEM((64, 64), F32),
        pltpu.VMEM((512, 256), F32),
        pltpu.VMEM((2, 16, NK), BF16),
        pltpu.VMEM((16, 2 * NK), I16),
        pltpu.VMEM((64, 2 * NK), BF16),
        dma((6,)),
        dma((11,)),
        dma((2,)),
        dma((2,)),
        dma((2,)),
        dma((5, 4)),
    ]
    results = pl.pallas_call(
        kernel,
        out_shape=(
            jax.ShapeDtypeStruct((128, 16, 256), F32),
            jax.ShapeDtypeStruct((32, 16, 256), F32),
            jax.ShapeDtypeStruct((4, 24, 256), F32),
            jax.ShapeDtypeStruct((16, 256), F32),
            jax.ShapeDtypeStruct((2, 4, 256), F32),
        ),
        in_specs=[hbm] * 6 + [vm] * 4,
        out_specs=(hbm,) * 5,
        scratch_shapes=scratch,
        compiler_params=pltpu.CompilerParams(
            vmem_limit_bytes=60 * 1024 * 1024, collective_id=0, has_side_effects=True
        ),
        name="coupled",
    )(flow, vel, heat, solid, cond, table.reshape(256, 1024), fp, sd, sp, b)
    return finish(*results)


def solution(mesh):
    placed = (
        P(None, ("grp", "dom"), None),
        P(None, None, ("grp", "dom"), None),
        P(None, ("grp", "dom"), None),
        P(None, ("grp", "dom"), None),
        P(None, ("grp", "dom"), None),
        P(),
        P(("grp", "dom")),
        P(("grp", "dom"), None),
        P(("grp", "dom")),
        P(("grp", "dom")),
    )
    return jax.shard_map(
        body,
        mesh=mesh,
        in_specs=placed,
        out_specs=(P(None, ("grp", "dom"), None), P(None, ("grp", "dom"), None)),
        check_vma=False,
    )
```
